8 devices in a mesh: part: 1 (over z), data: 2 (over y), stage: 4 (over x, core).
Axes of the slice: x: 2, y: 2, z: 1, core: 2. Of those that a mesh axis runs over, the one named last changes fastest.
Arguments:
- x_in: bfloat16 [32, 128, 2048], P(('part', 'data'))
- y_tgt: bfloat16 [32, 128, 2048], P(('part', 'data'))
- w_up: bfloat16 [4, 2048, 5632], P('stage')
- w_down: bfloat16 [4, 5632, 2048], P('stage')
- gain: float32 [4, 2048], P('stage')
Outputs:
- output 1: float32 [4, 2048, 5632], P(('part', 'stage'))
- output 2: float32 [4, 5632, 2048], P(('part', 'stage'))
- output 3: float32 [4, 2048], P(('part', 'stage'))
- output 4: float32 [1], P('part')
All inputs are finite; a program needn't handle non-finite values.
Results may differ from the reference program's by a relative error of at most 0.00258878.
Values are sent between devices in bfloat16 or wider.
A program may use at most 1 GiB of HBM per device.

```python
import jax
import jax.numpy as jnp
from jax import lax

MICRO_ALL = 32
TOKENS = 128
D = 2048
FF = 5632
LAYERS = 4
EPS = 1e-6
TOK_TOTAL = MICRO_ALL * TOKENS


def setup_inputs(seed: int = 0, part: int = 0) -> dict:
    base_key = jax.random.key(seed)
    key_up, key_down, key_gain, key_data = jax.random.split(base_key, 4)
    key_x, key_y = jax.random.split(jax.random.fold_in(key_data, part), 2)
    w_up = (jax.random.normal(key_up, (LAYERS, D, FF), jnp.float32) * D ** -0.5).astype(jnp.bfloat16)
    w_down = (jax.random.normal(key_down, (LAYERS, FF, D), jnp.float32) * FF ** -0.5).astype(jnp.bfloat16)
    gain = 1.0 + 0.25 * jax.random.normal(key_gain, (LAYERS, D), jnp.float32)
    x_in = jax.random.normal(key_x, (MICRO_ALL, TOKENS, D), jnp.float32).astype(jnp.bfloat16)
    y_tgt = jax.random.normal(key_y, (MICRO_ALL, TOKENS, D), jnp.float32).astype(jnp.bfloat16)
    return {"x_in": x_in, "y_tgt": y_tgt, "w_up": w_up, "w_down": w_down, "gain": gain}


def layer_fwd(x_rows, w_one, w_two, gain_row):
    x_float = x_rows.astype(jnp.float32)
    inv_rms = lax.rsqrt(jnp.mean(x_float * x_float, axis=-1, keepdims=True) + EPS)
    normed = (x_float * inv_rms * gain_row).astype(jnp.bfloat16)
    pre_act = jnp.dot(normed, w_one, preferred_element_type=jnp.float32)
    hidden = jax.nn.gelu(pre_act).astype(jnp.bfloat16)
    update = jnp.dot(hidden, w_two, preferred_element_type=jnp.float32)
    return (x_float + update).astype(jnp.bfloat16)


def layer_bwd(x_rows, d_out, w_one, w_two, gain_row):
    x_float = x_rows.astype(jnp.float32)
    inv_rms = lax.rsqrt(jnp.mean(x_float * x_float, axis=-1, keepdims=True) + EPS)
    unit_x = x_float * inv_rms
    normed = (unit_x * gain_row).astype(jnp.bfloat16)
    pre_act = jnp.dot(normed, w_one, preferred_element_type=jnp.float32)
    act_full, gelu_back = jax.vjp(jax.nn.gelu, pre_act)
    hidden = act_full.astype(jnp.bfloat16)
    g_two = jnp.dot(hidden.T, d_out, preferred_element_type=jnp.float32)
    d_hidden = jnp.dot(d_out, w_two.T, preferred_element_type=jnp.float32)
    d_pre = gelu_back(d_hidden)[0].astype(jnp.bfloat16)
    g_one = jnp.dot(normed.T, d_pre, preferred_element_type=jnp.float32)
    d_normed = jnp.dot(d_pre, w_one.T, preferred_element_type=jnp.float32)
    g_gain = jnp.sum(d_normed * unit_x, axis=0)
    d_unit = d_normed * gain_row
    d_x = inv_rms * (d_unit - unit_x * jnp.mean(d_unit * unit_x, axis=-1, keepdims=True))
    return (d_out.astype(jnp.float32) + d_x).astype(jnp.bfloat16), g_one, g_two, g_gain


def reference(x_in, y_tgt, w_up, w_down, gain):
    def micro_step(state_in, mb_pair):
        acc_one, acc_two, acc_gain, loss_sum = state_in
        x_now, y_now = mb_pair

        def fwd_body(hidden_x, layer_w):
            w_one, w_two, gain_row = layer_w
            return layer_fwd(hidden_x, w_one, w_two, gain_row), hidden_x

        top_out, saved_x = lax.scan(fwd_body, x_now, (w_up, w_down, gain))
        err_top = top_out.astype(jnp.float32) - y_now.astype(jnp.float32)
        d_top = (err_top / TOK_TOTAL).astype(jnp.bfloat16)

        def bwd_body(d_rows, layer_item):
            x_saved, w_one, w_two, gain_row = layer_item
            d_next, g_one, g_two, g_gain = layer_bwd(x_saved, d_rows, w_one, w_two, gain_row)
            return d_next, (g_one, g_two, g_gain)

        layer_grads = lax.scan(bwd_body, d_top, (saved_x, w_up, w_down, gain), reverse=True)[1]
        new_state = (acc_one + layer_grads[0], acc_two + layer_grads[1], acc_gain + layer_grads[2], loss_sum + jnp.sum(err_top * err_top))
        return new_state, None

    init_state = (jnp.zeros((LAYERS, D, FF), jnp.float32), jnp.zeros((LAYERS, FF, D), jnp.float32), jnp.zeros((LAYERS, D), jnp.float32), jnp.zeros((), jnp.float32))
    final_state = lax.scan(micro_step, init_state, (x_in, y_tgt))[0]
    d_up, d_down, d_gain, loss_sum = final_state
    loss_out = (loss_sum / (TOK_TOTAL * D)).reshape(1)
    return d_up, d_down, d_gain, loss_out
```

```python
import functools

import jax
import jax.numpy as jnp
from jax import lax
from jax.experimental import pallas as pl
from jax.experimental.pallas import tpu as pltpu
from jax.sharding import PartitionSpec as P

MESH = pl.DeviceIdType.MESH
EPS = 1e-6
C0 = 0.7978845608028654
C1 = 0.044715
ROWS = 256
TILE = 512
FWD, BWD, AUX = 0, 1, 2
LAST_DIMS = (((1,), (1,)), ((), ()))
ROW_DIMS = (((0,), (0,)), ((), ()))
F32 = jnp.float32
BF16 = jnp.bfloat16

ORDERS = (
    (
        "F0~", "F1", "F2", "F3", "F4", "F5", "F6", "F7", "F8",
        "B0~", "B1~", "A0", "B2~", "A1", "B3", "A2", "B4", "A3",
        "A4", "B5", "A5", "B6", "A6", "B7", "B8~",
    ),
    (
        "F0~", "F1~", "F2~", "F3~", "F4", "F5", "F6", "F7", "B0~",
        "F8", "B1~", "B2~", "B3~", "A0", "B4~", "A1", "A2", "B5",
        "A3", "B6", "A4", "B7", "A5", "B8", "A6",
    ),
    (
        "F0~", "F1~", "F2~", "F3~", "B0", "F4", "B1", "F5", "B2",
        "F6", "B3", "F7", "B4", "F8", "B5", "A0", "B6", "A1",
        "B7", "A2", "B8", "A3", "A4", "A5", "A6",
    ),
    (
        "F0~", "B0", "F1", "B1", "F2", "B2", "F3", "B3", "F4",
        "B4", "F5", "B5", "F6", "B6", "F7", "B7", "F8", "B8",
        "A0", "A1", "A2", "A3", "A4", "A5", "A6",
    ),
)
N_CHAIN = 9
N_OWN = 8
N_EXCH = 7


def gelu_and_grad(pre):
    sq = pre * pre
    th = jnp.tanh(pre * (C0 + (C0 * C1) * sq))
    cdf = 0.5 + 0.5 * th
    grad = cdf + (pre * (C0 + (3.0 * C0 * C1) * sq)) * (cdf * (1.0 - th))
    return pre * cdf, grad


def chain_kernel(orders, tok_total, x_in, y_tgt, w_up, w_down, gain, r_all, u_all, da_all, dh_all, gp_all, x_land, y_land,
                 dg_out, loss_out, w1, w2, main, rb, gp, ub, ring, dgp, dgr, lossacc, lossred, lossbuf,
                 w_ld, main_ld, rb_ld, r_sem, gp_o, gp_i, u_sem, dh_o, x_rcv, dh_rcv, rr_rcv, dd_rcv, y_rcv, dg_rcv, loss_rcv,
                 slot_snd, rr_snd, dd_snd, red_snd, dg_snd, loss_snd):
    n_items = len(orders[0])
    ff, d = w_down.shape
    me_y = lax.axis_index("data")
    sid = lax.axis_index("stage")
    other = 1 - me_y
    first, last = sid == 0, sid == 3
    f_tiles, d_tiles = ff // TILE, d // TILE
    cols = lambda k: pl.ds(k * TILE, TILE)

    def rows_of(chunk):
        return pl.ds(pl.multiple_of(chunk * ROWS, ROWS), ROWS)

    def own_chunk(idx):
        return jnp.where(idx < N_OWN, me_y * N_OWN + idx, other * N_OWN + idx - (N_CHAIN - N_OWN))

    def decode(step):
        code = jnp.int32(3)
        for stage_k, seq in enumerate(orders):
            val = jnp.int32(3)
            for step_k, item in enumerate(seq):
                val = jnp.where(step == step_k, item, val)
            code = jnp.where(sid == stage_k, val, code)
        return code

    def local(src, dst, sem):
        return pltpu.make_async_copy(src, dst, sem)

    def remote(src, dst, snd, rcv, **to):
        return pltpu.make_async_remote_copy(src, dst, snd, rcv, device_id=to, device_id_type=MESH)

    def relay_r(k):
        rows = rows_of(me_y * N_OWN + k)
        return remote(r_all.at[rows, :], r_all.at[rows, :], rr_snd.at[k], rr_rcv.at[k], data=other)

    def relay_dh(k):
        rows = rows_of(me_y * N_OWN + k)
        return remote(dh_all.at[rows, :], dh_all.at[rows, :], dd_snd.at[k], dd_rcv.at[k], data=other)

    def u_out(which, rows):
        dst = u_all if which == 0 else da_all
        return local(ub.at[which], dst.at[rows, :], u_sem.at[which, 0])

    f_part = (0, (f_tiles + 1) // 2, f_tiles)

    def aux_out(which, part, rows):
        dst = u_all if which == 0 else da_all
        lanes = pl.ds(f_part[part] * TILE, (f_part[part + 1] - f_part[part]) * TILE)
        return local(ub.at[which, :, lanes], dst.at[rows, lanes], u_sem.at[which, part])

    def wait_aux(part):
        for which in range(2):
            aux_out(which, part, pl.ds(0, ROWS)).wait()

    def wait_slot_send(slot):
        remote(main.at[slot], x_land.at[pl.ds(0, ROWS), :], slot_snd.at[slot], x_rcv.at[0], data=other).wait_send()

    def sends(code):
        kind = lax.rem(code, 4)
        return ((kind == FWD) & (sid < 3)) | ((kind == BWD) & (sid > 0))

    def load_x(idx, dst, sem):
        @pl.when(first & (idx < N_OWN))
        def _():
            local(x_in.at[rows_of(jnp.minimum(idx, N_OWN - 1)), :], dst, sem).start()

        @pl.when(jnp.logical_not(first & (idx < N_OWN)))
        def _():
            local(x_land.at[rows_of(idx), :], dst, sem).start()

    def prefetch(code, step, before, half):
        kind, idx = lax.rem(code, 4), lax.rem(code // 4, 16)
        slot = lax.rem(step, 3)

        @pl.when((step >= 3) & sends(before))
        def _():
            wait_slot_send(slot)

        @pl.when(kind == FWD)
        def _():
            @pl.when(jnp.logical_not(first & (idx < N_OWN)))
            def _():
                local(x_land.at[rows_of(idx), :], x_land.at[rows_of(idx), :], x_rcv.at[idx]).wait()

            @pl.when((step > 0) | jnp.logical_not(first))
            def _():
                load_x(idx, main.at[slot], main_ld.at[slot])

        @pl.when((kind == BWD) & jnp.logical_not(last))
        def _():
            rows = rows_of(own_chunk(idx))
            local(dh_all.at[rows, :], dh_all.at[rows, :], dh_rcv.at[idx]).wait()
            local(dh_all.at[rows, :], main.at[slot], main_ld.at[slot]).start()

            @pl.when(idx < N_EXCH)
            def _():
                relay_dh(idx).start()

        @pl.when(kind == AUX)
        def _():
            rows = rows_of(other * N_OWN + idx)
            local(r_all.at[rows, :], r_all.at[rows, :], rr_rcv.at[idx]).wait()
            local(r_all.at[rows, :], rb.at[half], rb_ld.at[half]).start()
            local(dh_all.at[rows, :], dh_all.at[rows, :], dd_rcv.at[idx]).wait()
            local(dh_all.at[rows, :], main.at[slot], main_ld.at[slot]).start()

    def load_gp(code):
        @pl.when((lax.rem(code, 4) == BWD) & jnp.logical_not(last))
        def _():
            local(gp_all.at[rows_of(lax.rem(code // 4, 16)), :], gp, gp_i).start()

    @pl.when(first)
    def _():
        local(x_in.at[pl.ds(0, ROWS), :], main.at[0], main_ld.at[0]).start()

    for k in range(2):
        half = pl.ds(k * (d // 2), d // 2)
        local(w_up.at[half, :], w1.at[half, :], w_ld.at[0]).start()
    for k in range(2):
        half = pl.ds(k * (ff // 2), ff // 2)
        local(w_down.at[half, :], w2.at[half, :], w_ld.at[1]).start()
    share = pl.ds(N_EXCH * ROWS, ROWS)
    share_x = remote(x_in.at[share, :], x_land.at[pl.ds(N_OWN * ROWS, ROWS), :], red_snd, x_rcv.at[N_OWN], data=other)
    share_y = remote(y_tgt.at[share, :], y_land, red_snd, y_rcv, data=other)

    @pl.when(first)
    def _():
        share_x.start()

    @pl.when(last)
    def _():
        share_y.start()

    dgp[...] = jnp.zeros_like(dgp)
    lossacc[...] = jnp.zeros_like(lossacc)
    for k in range(d // 128):
        rb[1, :, pl.ds(k * 128, 128)] = jnp.zeros((ROWS, 128), BF16)

    def run_fwd(step, idx, slot, nxt, early, before):
        @pl.when(last)
        def _():
            @pl.when(idx < N_OWN)
            def _():
                local(y_tgt.at[rows_of(jnp.minimum(idx, N_OWN - 1)), :], rb.at[1], rb_ld.at[1]).start()

            @pl.when(idx >= N_OWN)
            def _():
                local(y_land, y_land, y_rcv).wait()
                local(y_land, rb.at[1], rb_ld.at[1]).start()

        local(x_in.at[pl.ds(0, ROWS), :], main.at[slot], main_ld.at[slot]).wait()
        part_rows = ROWS // 4
        for h in range(4):
            rws = pl.ds(h * part_rows, part_rows)
            acc = jnp.zeros((part_rows, 128), F32)
            for k in range(d // 128):
                xk = main[slot, rws, pl.ds(k * 128, 128)].astype(F32)
                acc = acc + xk * xk
            q = lax.rsqrt(jnp.sum(acc, axis=-1, keepdims=True) * (1.0 / d) + EPS)
            for k in range(d // 128):
                lanes = pl.ds(k * 128, 128)
                rb[0, rws, lanes] = (main[slot, rws, lanes].astype(F32) * q * gain[:, lanes]).astype(BF16)
        rows = rows_of(own_chunk(idx))
        r_out = local(rb.at[0], r_all.at[rows, :], r_sem)
        r_out.start()

        @pl.when(step == 0)
        def _():
            local(w_up, w1, w_ld.at[0]).wait()

        for k in range(f_tiles + 1):
            if k > 0:
                act, grad = gelu_and_grad(ring[(k - 1) % 2])
                ub[0, :, cols(k - 1)] = act.astype(BF16)
                gp[:, cols(k - 1)] = grad
            if k < f_tiles:
                ring[k % 2] = jnp.dot(rb[0], w1[:, cols(k)], preferred_element_type=F32)
        r_out.wait()

        @pl.when(idx < N_EXCH)
        def _():
            relay_r(jnp.minimum(idx, N_EXCH - 1)).start()

        u_out(0, rows).start()
        gp_out = local(gp, gp_all.at[rows_of(idx), :], gp_o)

        @pl.when(jnp.logical_not(last))
        def _():
            gp_out.start()

        @pl.when(step == 0)
        def _():
            local(w_down, w2, w_ld.at[1]).wait()

        @pl.when(last)
        def _():
            local(y_land, rb.at[1], rb_ld.at[1]).wait()

        out_slot = jnp.where(last, lax.rem(step + 1, 3), slot)
        count = last & (idx < N_OWN)

        def h_done(k):
            h = (main[slot, :, cols(k)].astype(F32) + ring[(f_tiles + k) % 2]).astype(BF16)
            err = h.astype(F32) - rb[1, :, cols(k)].astype(F32)
            main[out_slot, :, cols(k)] = jnp.where(last, (err * (1.0 / tok_total)).astype(BF16), h)
            part = jnp.sum((err * err).reshape(ROWS // 8, 8, TILE), axis=0)
            lossacc[:, cols(k)] += jnp.where(count, part, 0.0)

        def h_tiles(lo, hi):
            for k in range(lo, hi + 1):
                if k > lo:
                    h_done(k - 1)
                if k < hi:
                    ring[(f_tiles + k) % 2] = jnp.dot(ub[0], w2[:, cols(k)], preferred_element_type=F32)

        def send_half(k):
            lanes = pl.ds(k * (d // 2), d // 2)

            @pl.when(sid < 3)
            def _():
                remote(main.at[slot, :, lanes], x_land.at[rows_of(idx), lanes], slot_snd.at[slot], x_rcv.at[idx],
                       stage=jnp.minimum(sid + 1, 3)).start()

        h_tiles(0, d_tiles // 2)
        send_half(0)
        u_out(0, rows).wait()

        @pl.when(jnp.logical_not(last))
        def _():
            gp_out.wait()

        load_gp(nxt)

        @pl.when(early)
        def _():
            prefetch(nxt, step + 1, before, 0)

        h_tiles(d_tiles // 2, d_tiles)
        send_half(1)

    def run_bwd(step, idx, slot, nxt, early, before):
        load_x(idx, rb.at[1], rb_ld.at[1])
        rows = rows_of(own_chunk(idx))
        dh_out = local(main.at[slot], dh_all.at[rows, :], dh_o)

        @pl.when(last)
        def _():
            dh_out.start()

        @pl.when(jnp.logical_not(last))
        def _():
            local(x_in.at[pl.ds(0, ROWS), :], main.at[slot], main_ld.at[slot]).wait()
            local(gp_all.at[pl.ds(0, ROWS), :], gp, gp_i).wait()

        for k in range(f_tiles):
            du = lax.dot_general(main[slot], w2[cols(k), :], LAST_DIMS, preferred_element_type=F32)
            ub[1, :, cols(k)] = (du * gp[:, cols(k)]).astype(BF16)
        u_out(1, rows).start()

        @pl.when(last)
        def _():
            dh_out.wait()

            @pl.when(idx < N_EXCH)
            def _():
                relay_dh(jnp.minimum(idx, N_EXCH - 1)).start()

        local(x_land.at[pl.ds(0, ROWS), :], rb.at[1], rb_ld.at[1]).wait()

        def r_done(k):
            sq = jnp.zeros((ROWS, 128), F32)
            pr = jnp.zeros((ROWS, 128), F32)
            for j in range(TILE // 128):
                lanes = pl.ds(k * TILE + j * 128, 128)
                xk = rb[1, :, lanes].astype(F32)
                sq = sq + xk * xk
                pr = pr + gp[:, lanes] * gain[:, lanes] * xk
            sums = (pl.ds(0, ROWS), pl.ds(0, 128))
            ring[0, *sums] = sq if k == 0 else ring[0, *sums] + sq
            ring[1, *sums] = pr if k == 0 else ring[1, *sums] + pr

        def r_tiles(lo, hi):
            for k in range(lo, hi + 1):
                if k > lo:
                    r_done(k - 1)
                if k < hi:
                    gp[:, cols(k)] = lax.dot_general(ub[1], w1[cols(k), :], LAST_DIMS, preferred_element_type=F32)

        r_tiles(0, d_tiles // 2)
        u_out(1, rows).wait()

        @pl.when(early)
        def _():
            prefetch(nxt, step + 1, before, 0)

        r_tiles(d_tiles // 2, d_tiles)
        keep = idx < N_OWN
        half = ROWS // 4
        for h in range(4):
            rws = pl.ds(h * half, half)
            q = lax.rsqrt(jnp.sum(ring[0, rws, pl.ds(0, 128)], axis=-1, keepdims=True) * (1.0 / d) + EPS)
            mean = q * jnp.sum(ring[1, rws, pl.ds(0, 128)], axis=-1, keepdims=True) * (1.0 / d)
            qqm = q * q * mean
            for k in range(d // 128):
                lanes = pl.ds(k * 128, 128)
                xk = rb[1, rws, lanes].astype(F32)
                drk = gp[rws, lanes]
                dhk = main[slot, rws, lanes].astype(F32)
                main[slot, rws, lanes] = (dhk + (q * (drk * gain[:, lanes]) - xk * qqm)).astype(BF16)
                part = jnp.sum((drk * (xk * q)).reshape(half // 8, 8, 128), axis=0)
                dgp[:, lanes] += jnp.where(keep, part, 0.0)

        @pl.when(sid > 0)
        def _():
            remote(main.at[slot], dh_all.at[rows, :], slot_snd.at[slot], dh_rcv.at[idx],
                   stage=jnp.maximum(sid - 1, 0)).start()

        load_gp(nxt)

        @pl.when(idx == N_CHAIN - 1)
        def _():
            remote(dgp, dgr, dg_snd, dg_rcv, data=other).start()

            @pl.when(last)
            def _():
                red = lossacc[:, pl.ds(0, 128)]
                for k in range(1, d // 128):
                    red = red + lossacc[:, pl.ds(k * 128, 128)]
                lossred[...] = red
                for hop in range(1, 4):
                    remote(lossred, lossbuf.at[me_y], loss_snd.at[hop - 1], loss_rcv.at[me_y], stage=3 - hop).start()
                for hop in range(4):
                    remote(lossred, lossbuf.at[me_y], loss_snd.at[3 + hop], loss_rcv.at[me_y],
                           data=other, stage=3 - hop).start()

    def run_aux(step, idx, slot, nxt, early, before, half, after_aux):
        load_gp(nxt)
        local(r_all.at[pl.ds(0, ROWS), :], rb.at[half], rb_ld.at[half]).wait()
        local(x_in.at[pl.ds(0, ROWS), :], main.at[slot], main_ld.at[slot]).wait()
        rows = rows_of(other * N_OWN + idx)

        def tiles(lo, hi):
            for k in range(lo, hi + 1):
                if k > lo:
                    act, grad = gelu_and_grad(ring[(k - 1) % 2])
                    ub[0, :, cols(k - 1)] = act.astype(BF16)
                    ub[1, :, cols(k - 1)] = (du * grad).astype(BF16)
                if k < hi:
                    ring[k % 2] = jnp.dot(rb[half], w1[:, cols(k)], preferred_element_type=F32)
                    du = lax.dot_general(main[slot], w2[cols(k), :], LAST_DIMS, preferred_element_type=F32)
            for which in range(2):
                aux_out(which, int(lo > 0), rows).start()

        tiles(0, f_part[1])

        @pl.when(after_aux)
        def _():
            wait_aux(1)

        @pl.when(early)
        def _():
            prefetch(nxt, step + 1, before, 1 - half)

        tiles(f_part[1], f_tiles)

    def item(step, carry):
        b3, b2, b1, cur, was = carry
        half = jnp.where(lax.rem(b1, 4) == AUX, 1 - was, 0)
        nxt = decode(step + 1)
        kind, idx = lax.rem(cur, 4), lax.rem(cur // 4, 16)
        slot = lax.rem(step, 3)
        early = (step + 1 < n_items) & (lax.rem(nxt // 64, 2) == 1)

        @pl.when(lax.rem(cur // 64, 2) == 0)
        def _():
            prefetch(cur, step, b3, half)

        after_aux = lax.rem(b1, 4) == AUX

        @pl.when(after_aux)
        def _():
            wait_aux(0)

        @pl.when(after_aux & (kind != AUX))
        def _():
            wait_aux(1)

        @pl.when(kind == FWD)
        def _():
            run_fwd(step, idx, slot, nxt, early, b2)

        @pl.when(kind == BWD)
        def _():
            run_bwd(step, idx, slot, nxt, early, b2)

        @pl.when(kind == AUX)
        def _():
            run_aux(step, idx, slot, nxt, early, b2, half, after_aux)

        return b2, b1, cur, nxt, half

    none = jnp.int32(3)
    b3, b2, b1, _, _ = lax.fori_loop(0, n_items, item, (none, none, none, decode(0), jnp.int32(0)))

    @pl.when(lax.rem(b1, 4) == AUX)
    def _():
        wait_aux(0)
        wait_aux(1)

    for back, code in ((3, b3), (2, b2), (1, b1)):
        @pl.when(sends(code))
        def _():
            wait_slot_send((n_items - back) % 3)

    def end_relays(k, carry):
        relay_r(k).wait_send()
        relay_dh(k).wait_send()
        return carry

    lax.fori_loop(0, N_EXCH, end_relays, 0)

    @pl.when(first)
    def _():
        share_x.wait_send()

    @pl.when(last)
    def _():
        share_y.wait_send()

    dg_copy = remote(dgp, dgr, dg_snd, dg_rcv, data=other)
    dg_copy.wait_send()
    dg_copy.wait_recv()
    dg_out[...] = jnp.sum(dgp[...] + dgr[...], axis=0, keepdims=True)

    @pl.when(last)
    def _():
        for hop in range(7):
            remote(lossred, lossbuf.at[me_y], loss_snd.at[hop], loss_rcv.at[me_y], data=other).wait_send()
        lossbuf[me_y] = lossred[...]

    @pl.when(jnp.logical_not(last))
    def _():
        local(lossred, lossbuf.at[me_y], loss_rcv.at[me_y]).wait()

    local(lossred, lossbuf.at[other], loss_rcv.at[other]).wait()
    loss_out[0] = jnp.sum(lossbuf[0] + lossbuf[1]) / (tok_total * d)


def encode(order):
    seq = []
    for name in order:
        kind = "FBA".index(name[0])
        seq.append(kind + 4 * int(name[1:].rstrip("~")) + 64 * int(not name.endswith("~")))
    return tuple(seq)


def solution(mesh):
    n_data = mesh.shape["data"]
    orders = tuple(encode(order) for order in ORDERS)

    def local_step(x_in, y_tgt, w_up, w_down, gain):
        n_micro, tokens, d = x_in.shape
        ff = w_up.shape[2]
        own = n_micro * tokens
        total = n_data * own
        x_rows, y_rows = x_in.reshape(own, d), y_tgt.reshape(own, d)
        hbm = pl.BlockSpec(memory_space=pl.ANY)
        vmem = pl.BlockSpec(memory_space=pltpu.VMEM)
        dma, sem = pltpu.SemaphoreType.DMA, pltpu.SemaphoreType.DMA(())
        out = pl.pallas_call(
            functools.partial(chain_kernel, orders, total),
            out_shape=(
                jax.ShapeDtypeStruct((total, d), BF16),
                jax.ShapeDtypeStruct((total, ff), BF16),
                jax.ShapeDtypeStruct((total, ff), BF16),
                jax.ShapeDtypeStruct((total, d), BF16),
                jax.ShapeDtypeStruct((N_CHAIN * ROWS, ff), F32),
                jax.ShapeDtypeStruct((N_CHAIN * ROWS, d), BF16),
                jax.ShapeDtypeStruct((ROWS, d), BF16),
                jax.ShapeDtypeStruct((1, d), F32),
                jax.ShapeDtypeStruct((1,), F32),
            ),
            in_specs=[hbm, hbm, hbm, hbm, vmem],
            out_specs=[hbm] * 7 + [vmem, pl.BlockSpec(memory_space=pltpu.SMEM)],
            scratch_shapes=[
                pltpu.VMEM((d, ff), BF16),
                pltpu.VMEM((ff, d), BF16),
                pltpu.VMEM((3, ROWS, d), BF16),
                pltpu.VMEM((2, ROWS, d), BF16),
                pltpu.VMEM((ROWS, ff), F32),
                pltpu.VMEM((2, ROWS, ff), BF16),
                pltpu.VMEM((2, ROWS, TILE), F32),
                pltpu.VMEM((8, d), F32),
                pltpu.VMEM((8, d), F32),
                pltpu.VMEM((8, d), F32),
                pltpu.VMEM((8, 128), F32),
                pltpu.VMEM((2, 8, 128), F32),
                dma((2,)), dma((3,)), dma((2,)), sem, sem, sem, dma((2, 2)), sem,
                dma((N_CHAIN,)), dma((N_CHAIN,)), dma((N_EXCH,)), dma((N_EXCH,)), sem, sem, dma((2,)),
                dma((3,)), dma((N_EXCH,)), dma((N_EXCH,)), sem, sem, dma((7,)),
            ],
            compiler_params=pltpu.CompilerParams(has_side_effects=True, vmem_limit_bytes=67043328),
            name="chain",
        )(x_rows, y_rows, w_up[0], w_down[0], gain)
        r_all, u_all, da_all, dh_all = out[:4]
        d_up = lax.dot_general(r_all, da_all, ROW_DIMS, preferred_element_type=F32)
        d_down = lax.dot_general(u_all, dh_all, ROW_DIMS, preferred_element_type=F32)
        return d_up[None], d_down[None], out[7], out[8]

    return jax.shard_map(local_step, mesh=mesh, in_specs=(P(("part", "data"), None, None), P(("part", "data"), None, None), P("stage", None, None), P("stage", None, None), P("stage", None)), out_specs=(P(("part", "stage"), None, None), P(("part", "stage"), None, None), P(("part", "stage"), None), P("part")), check_vma=False)
```

```python
import functools

import jax
import jax.numpy as jnp
from jax import lax
from jax.experimental import pallas as pl
from jax.experimental.pallas import tpu as pltpu
from jax.sharding import PartitionSpec as P

MESH = pl.DeviceIdType.MESH
EPS = 1e-6
C0 = 0.7978845608028654
C1 = 0.044715
ROWS = 256
HALF = ROWS // 2
TILE = 512
FWD, BWD, AUX, PRE = 0, 1, 2, 3
NONE = 64 * 17
LAST_DIMS = (((1,), (1,)), ((), ()))
ROW_DIMS = (((0,), (0,)), ((), ()))
F32 = jnp.float32
BF16 = jnp.bfloat16

ORDERS = (
    (
        "P0~", "P1", "P2", "P3", "F2", "F3", "F4", "F5", "F6",
        "F7", "F8", "B0~", "B1~", "B2~", "A0", "A1", "A2~", "B3",
        "B4", "A3", "A4", "B5", "B6", "A5", "A6", "B7", "B8",
    ),
    (
        "P0~", "P1~", "P2", "P3", "F2~", "F3~", "F4~", "F5", "B0",
        "F6", "F7", "B1", "B2~", "A0", "F8", "B3", "B4~", "A1",
        "A2", "B5", "B6~", "A3", "A4", "B7~", "B8", "A5", "A6",
    ),
    (
        "P0~", "P1~", "P2~", "P3~", "B0~", "F2", "F3", "B1", "F4",
        "B2", "F5", "B3", "F6", "B4", "F7", "B5", "F8", "B6",
        "A0", "A1", "B7", "B8", "A2", "A3", "A4", "A5", "A6",
    ),
    (
        "P0~", "P1~", "B0", "P2", "P3", "B1", "F2~", "B2", "F3",
        "B3", "F4", "B4", "F5", "B5", "F6", "B6", "F7", "B7",
        "F8", "B8", "A0", "A1", "A2", "A3", "A4", "A5", "A6",
    ),
)
N_CHAIN = 9
N_OWN = 8
N_EXCH = 7
N_PRE = 2


def gelu_and_grad(pre):
    sq = pre * pre
    th = jnp.tanh(pre * (C0 + (C0 * C1) * sq))
    cdf = 0.5 + 0.5 * th
    grad = cdf + (pre * (C0 + (3.0 * C0 * C1) * sq)) * (cdf * (1.0 - th))
    return pre * cdf, grad


def chain_kernel(orders, tok_total, x_in, y_tgt, w_up, w_down, gain, r_all, u_all, da_all, dh_all, gp_all, x_land, y_land,
                 dg_out, loss_out, w1, w2, main, rb, gp, ub, ring, dgp, dgr, lossacc, lossred, lossbuf,
                 w_ld, main_ld, rb_ld, r_sem, gp_o, gp_i, u_sem, dh_o, x_rcv, dh_rcv, rr_rcv, dd_rcv, y_rcv, dg_rcv, loss_rcv,
                 slot_snd, rr_snd, dd_snd, red_snd, dg_snd, loss_snd):
    n_items = len(orders[0])
    ff, d = w_down.shape
    me_y = lax.axis_index("data")
    sid = lax.axis_index("stage")
    other = 1 - me_y
    first, last = sid == 0, sid == 3
    f_tiles, d_tiles = ff // TILE, d // TILE
    cols = lambda k: pl.ds(k * TILE, TILE)

    def rows_of(chunk):
        return pl.ds(pl.multiple_of(chunk * ROWS, ROWS), ROWS)

    def own_chunk(idx):
        return jnp.where(idx < N_OWN, me_y * N_OWN + idx, other * N_OWN + idx - (N_CHAIN - N_OWN))

    def decode(step):
        code = jnp.int32(NONE)
        for stage_k, seq in enumerate(orders):
            val = jnp.int32(NONE)
            for step_k, item in enumerate(seq):
                val = jnp.where(step == step_k, item, val)
            code = jnp.where(sid == stage_k, val, code)
        return code

    def fields(code):
        kind, idx = lax.rem(code, 4), lax.rem(code // 4, 16)
        return jnp.where(code >= NONE, -1, kind), idx, lax.rem(code // 64, 2) == 1

    def local(src, dst, sem):
        return pltpu.make_async_copy(src, dst, sem)

    def remote(src, dst, snd, rcv, **to):
        return pltpu.make_async_remote_copy(src, dst, snd, rcv, device_id=to, device_id_type=MESH)

    def relay_r(k):
        rows = rows_of(me_y * N_OWN + k)
        return remote(r_all.at[rows, :], r_all.at[rows, :], rr_snd.at[k], rr_rcv.at[k], data=other)

    def relay_dh(k):
        rows = rows_of(me_y * N_OWN + k)
        return remote(dh_all.at[rows, :], dh_all.at[rows, :], dd_snd.at[k], dd_rcv.at[k], data=other)

    def u_out(which, rows):
        dst = u_all if which == 0 else da_all
        return local(ub.at[which], dst.at[rows, :], u_sem.at[which])

    def sends(code):
        kind = fields(code)[0]
        return (((kind == FWD) | (kind == PRE)) & (sid < 3)) | ((kind == BWD) & (sid > 0))

    def wait_slot_send(code, slot):
        pre = fields(code)[0] == PRE

        @pl.when(sends(code) & pre)
        def _():
            half = pl.ds(0, HALF)
            remote(main.at[slot, half, :], x_land.at[half, :], slot_snd.at[slot], x_rcv.at[0], data=other).wait_send()

        @pl.when(sends(code) & jnp.logical_not(pre))
        def _():
            remote(main.at[slot], x_land.at[pl.ds(0, ROWS), :], slot_snd.at[slot], x_rcv.at[0], data=other).wait_send()

    def load_x(idx, dst, sem):
        @pl.when(first & (idx < N_OWN))
        def _():
            local(x_in.at[rows_of(jnp.minimum(idx, N_OWN - 1)), :], dst, sem).start()

        @pl.when(jnp.logical_not(first & (idx < N_OWN)))
        def _():
            local(x_land.at[rows_of(idx), :], dst, sem).start()

    def prefetch(code, step, before, waited=None):
        kind, idx, _ = fields(code)
        slot = lax.rem(step, 3)

        if waited is None:
            wait_slot_send(before, slot)
        else:
            @pl.when(jnp.logical_not(waited))
            def _():
                wait_slot_send(before, slot)

        @pl.when(kind == PRE)
        def _():
            half = pl.ds(pl.multiple_of(idx * HALF, HALF), HALF)
            dst = main.at[slot, in_chunk(idx), :]

            @pl.when(first & (step > 0))
            def _():
                local(x_in.at[half, :], dst, main_ld.at[slot]).start()

            @pl.when(jnp.logical_not(first))
            def _():
                local(x_land.at[half, :], x_land.at[half, :], x_rcv.at[pre_sem(idx)]).wait()
                local(x_land.at[half, :], dst, main_ld.at[slot]).start()

        @pl.when(kind == FWD)
        def _():
            @pl.when(jnp.logical_not(first & (idx < N_OWN)))
            def _():
                local(x_land.at[rows_of(idx), :], x_land.at[rows_of(idx), :], x_rcv.at[idx]).wait()

            load_x(idx, main.at[slot], main_ld.at[slot])

        @pl.when((kind == BWD) & jnp.logical_not(last))
        def _():
            rows = rows_of(own_chunk(idx))
            local(dh_all.at[rows, :], dh_all.at[rows, :], dh_rcv.at[idx]).wait()
            local(dh_all.at[rows, :], main.at[slot], main_ld.at[slot]).start()

            @pl.when(idx < N_EXCH)
            def _():
                relay_dh(idx).start()

        @pl.when(kind == AUX)
        def _():
            rows = rows_of(other * N_OWN + idx)
            local(r_all.at[rows, :], r_all.at[rows, :], rr_rcv.at[idx]).wait()
            local(r_all.at[rows, :], rb.at[0], rb_ld.at[0]).start()
            local(dh_all.at[rows, :], dh_all.at[rows, :], dd_rcv.at[idx]).wait()
            local(dh_all.at[rows, :], main.at[slot], main_ld.at[slot]).start()

    def pre_sem(idx):
        return jnp.where(lax.rem(idx, 2) == 0, N_CHAIN + idx // 2, idx // 2)

    def in_chunk(idx):
        return pl.ds(pl.multiple_of(lax.rem(idx, 2) * HALF, HALF), HALF)

    def load_gp(code, lo=0, hi=None):
        kind, idx, _ = fields(code)
        lanes = pl.ds(lo, (hi or ff) - lo)

        @pl.when((kind == BWD) & jnp.logical_not(last))
        def _():
            local(gp_all.at[rows_of(idx), lanes], gp.at[:, lanes], gp_i).start()

    def normalise(slot, rws):
        acc = jnp.zeros((rws.size, 128), F32)
        for k in range(d // 128):
            xk = main[slot, rws, pl.ds(k * 128, 128)].astype(F32)
            acc = acc + xk * xk
        q = lax.rsqrt(jnp.sum(acc, axis=-1, keepdims=True) * (1.0 / d) + EPS)
        for k in range(d // 128):
            lanes = pl.ds(k * 128, 128)
            rb[0, rws, lanes] = (main[slot, rws, lanes].astype(F32) * q * gain[:, lanes]).astype(BF16)

    def up_tiles(rws):
        n = rws.size
        for k in range(f_tiles + 1):
            if k > 0:
                act, grad = gelu_and_grad(ring[(k - 1) % 2, pl.ds(0, n), :])
                ub[0, rws, cols(k - 1)] = act.astype(BF16)
                gp[rws, cols(k - 1)] = grad
            if k < f_tiles:
                ring[k % 2, pl.ds(0, n), :] = jnp.dot(rb[0, rws, :], w1[:, cols(k)], preferred_element_type=F32)

    def down_tiles(lo, hi, slot, out_slot, rws, count):
        n = rws.size
        for k in range(lo, hi + 1):
            if k > lo:
                upd = ring[(k - 1) % 2, pl.ds(0, n), :]
                h = (main[slot, rws, cols(k - 1)].astype(F32) + upd).astype(BF16)
                err = h.astype(F32) - rb[1, rws, cols(k - 1)].astype(F32)
                main[out_slot, rws, cols(k - 1)] = jnp.where(last, (err * (1.0 / tok_total)).astype(BF16), h)
                part = jnp.sum((err * err).reshape(n // 8, 8, TILE), axis=0)
                lossacc[:, cols(k - 1)] += jnp.where(count, part, 0.0)
            if k < hi:
                ring[k % 2, pl.ds(0, n), :] = jnp.dot(ub[0, rws, :], w2[:, cols(k)], preferred_element_type=F32)

    @pl.when(first)
    def _():
        half = pl.ds(0, HALF)
        local(x_in.at[half, :], main.at[0, half, :], main_ld.at[0]).start()

    for k in range(2):
        half = pl.ds(k * (d // 2), d // 2)
        local(w_up.at[half, :], w1.at[half, :], w_ld.at[0]).start()
    def load_w2(k):
        lanes = pl.ds(k * (d // 2), d // 2)
        return local(w_down.at[:, lanes], w2.at[:, lanes], w_ld.at[1 + k])

    @pl.when(jnp.logical_not(first))
    def _():
        for k in range(2):
            load_w2(k).start()

    share = pl.ds(N_EXCH * ROWS, ROWS)
    share_x = remote(x_in.at[share, :], x_land.at[pl.ds(N_OWN * ROWS, ROWS), :], red_snd, x_rcv.at[N_OWN], data=other)
    share_y = remote(y_tgt.at[share, :], y_land, red_snd, y_rcv, data=other)

    @pl.when(first)
    def _():
        share_x.start()

    @pl.when(last)
    def _():
        share_y.start()

    dgp[...] = jnp.zeros_like(dgp)
    lossacc[...] = jnp.zeros_like(lossacc)
    for k in range(d // 128):
        rb[1, :, pl.ds(k * 128, 128)] = jnp.zeros((ROWS, 128), BF16)

    d_half = d_tiles // 2

    def send_half(k, slot, rws, land, sem):
        lanes = pl.ds(k * (d // 2), d // 2)

        @pl.when(sid < 3)
        def _():
            remote(main.at[slot, rws, lanes], x_land.at[land, lanes], slot_snd.at[slot], x_rcv.at[sem],
                   stage=jnp.minimum(sid + 1, 3)).start()

    def run_pre(step, idx, slot, nxt, early, before, prev):
        rws, at = in_chunk(idx), pl.ds(pl.multiple_of(idx * HALF, HALF), HALF)
        odd = lax.rem(idx, 2)
        own = pl.ds(pl.multiple_of(me_y * N_OWN * ROWS + idx * HALF, HALF), HALF)

        @pl.when(last)
        def _():
            local(y_tgt.at[at, :], rb.at[1, rws, :], rb_ld.at[1]).start()

        local(x_in.at[pl.ds(0, HALF), :], main.at[slot, rws, :], main_ld.at[slot]).wait()
        for h in range(2):
            normalise(slot, pl.ds(pl.multiple_of(odd * HALF + h * (HALF // 2), HALF // 2), HALF // 2))
        r_out = local(rb.at[0, rws, :], r_all.at[own, :], r_sem)
        r_out.start()

        @pl.when(step == 0)
        def _():
            local(w_up, w1, w_ld.at[0]).wait()

        @pl.when((step == 0) & first)
        def _():
            for k in range(2):
                load_w2(k).start()

        up_tiles(rws)
        r_out.wait()

        @pl.when(odd == 1)
        def _():
            relay_r(idx // 2).start()

        act_out = local(ub.at[0, rws, :], u_all.at[own, :], u_sem.at[0])
        act_out.start()
        gp_out = local(gp.at[rws, :], gp_all.at[at, :], gp_o)

        @pl.when(jnp.logical_not(last))
        def _():
            gp_out.start()

        @pl.when(step == 0)
        def _():
            load_w2(0).wait()

        @pl.when(last)
        def _():
            local(y_tgt.at[at, :], rb.at[1, rws, :], rb_ld.at[1]).wait()

        out_slot = jnp.where(last, lax.rem(step + 2 - odd, 3), slot)

        @pl.when(last & (odd == 0))
        def _():
            wait_slot_send(prev, out_slot)

        down_tiles(0, d_half, slot, out_slot, rws, last)
        send_half(0, slot, rws, at, pre_sem(idx))
        act_out.wait()

        @pl.when(jnp.logical_not(last))
        def _():
            gp_out.wait()

        load_gp(nxt)

        @pl.when(early)
        def _():
            prefetch(nxt, step + 1, before, last & (odd == 1))

        @pl.when(step == 0)
        def _():
            load_w2(1).wait()

        down_tiles(d_half, d_tiles, slot, out_slot, rws, last)
        send_half(1, slot, rws, at, pre_sem(idx))

    def up_phase(step, kind, idx, slot, rows):
        fwd = kind == FWD
        r_out = local(rb.at[0], r_all.at[rows, :], r_sem)
        gp_out = local(gp, gp_all.at[rows_of(idx), :], gp_o)

        @pl.when(fwd & last)
        def _():
            @pl.when(idx < N_OWN)
            def _():
                local(y_tgt.at[rows_of(jnp.minimum(idx, N_OWN - 1)), :], rb.at[1], rb_ld.at[1]).start()

            @pl.when(idx >= N_OWN)
            def _():
                local(y_land, y_land, y_rcv).wait()
                local(y_land, rb.at[1], rb_ld.at[1]).start()

        @pl.when(fwd)
        def _():
            local(x_in.at[pl.ds(0, ROWS), :], main.at[slot], main_ld.at[slot]).wait()
            for h in range(4):
                normalise(slot, pl.ds(h * (ROWS // 4), ROWS // 4))
            r_out.start()

        @pl.when(kind == AUX)
        def _():
            local(r_all.at[pl.ds(0, ROWS), :], rb.at[0], rb_ld.at[0]).wait()

        up_tiles(pl.ds(0, ROWS))
        u_out(0, rows).start()

        @pl.when(fwd)
        def _():
            r_out.wait()

        @pl.when(fwd & (idx < N_EXCH))
        def _():
            relay_r(jnp.minimum(idx, N_EXCH - 1)).start()

        @pl.when(fwd & jnp.logical_not(last))
        def _():
            gp_out.start()

    def down_phase(step, idx, slot, nxt, early, before, after_aux):
        @pl.when(last)
        def _():
            local(y_land, rb.at[1], rb_ld.at[1]).wait()

        out_slot = jnp.where(last, lax.rem(step + 1, 3), slot)
        count = last & (idx < N_OWN)
        every = pl.ds(0, ROWS)
        down_tiles(0, d_half, slot, out_slot, every, count)
        send_half(0, slot, every, rows_of(idx), idx)
        u_out(0, every).wait()

        @pl.when(after_aux)
        def _():
            u_out(1, every).wait()

        @pl.when(jnp.logical_not(last))
        def _():
            local(gp, gp_all.at[every, :], gp_o).wait()

        load_gp(nxt)

        @pl.when(early)
        def _():
            prefetch(nxt, step + 1, before)

        down_tiles(d_half, d_tiles, slot, out_slot, every, count)
        send_half(1, slot, every, rows_of(idx), idx)

    def back_phase(step, kind, idx, slot, rows, nxt, early, before, after_aux):
        bwd, aux = kind == BWD, kind == AUX
        dh_out = local(main.at[slot], dh_all.at[rows, :], dh_o)

        @pl.when(bwd)
        def _():
            load_x(idx, rb.at[1], rb_ld.at[1])

        @pl.when(bwd & last)
        def _():
            dh_out.start()

        @pl.when(aux | jnp.logical_not(last))
        def _():
            local(x_in.at[pl.ds(0, ROWS), :], main.at[slot], main_ld.at[slot]).wait()

        @pl.when(bwd & jnp.logical_not(last))
        def _():
            local(gp_all.at[pl.ds(0, ROWS), :], gp, gp_i).wait()

        @pl.when(after_aux)
        def _():
            u_out(1, rows).wait()

        @pl.when(aux & early)
        def _():
            prefetch(nxt, step + 1, before)

        for k in range(f_tiles):
            du = lax.dot_general(main[slot], w2[cols(k), :], LAST_DIMS, preferred_element_type=F32)
            ub[1, :, cols(k)] = (du * gp[:, cols(k)]).astype(BF16)
        u_out(1, rows).start()

        @pl.when(aux)
        def _():
            u_out(0, rows).wait()
            load_gp(nxt)

        @pl.when(bwd & last)
        def _():
            dh_out.wait()

        @pl.when(bwd & last & (idx < N_EXCH))
        def _():
            relay_dh(jnp.minimum(idx, N_EXCH - 1)).start()

    def grad_phase(step, idx, slot, rows, nxt, early, before):
        local(x_land.at[pl.ds(0, ROWS), :], rb.at[1], rb_ld.at[1]).wait()

        def r_done(k):
            sq = jnp.zeros((ROWS, 128), F32)
            pr = jnp.zeros((ROWS, 128), F32)
            for j in range(TILE // 128):
                lanes = pl.ds(k * TILE + j * 128, 128)
                xk = rb[1, :, lanes].astype(F32)
                sq = sq + xk * xk
                pr = pr + gp[:, lanes] * gain[:, lanes] * xk
            sums = (pl.ds(0, ROWS), pl.ds(0, 128))
            ring[0, *sums] = sq if k == 0 else ring[0, *sums] + sq
            ring[1, *sums] = pr if k == 0 else ring[1, *sums] + pr

        def r_tiles(lo, hi):
            for k in range(lo, hi + 1):
                if k > lo:
                    r_done(k - 1)
                if k < hi:
                    gp[:, cols(k)] = lax.dot_general(ub[1], w1[cols(k), :], LAST_DIMS, preferred_element_type=F32)

        r_tiles(0, d_half)
        u_out(1, rows).wait()
        load_gp(nxt, lo=d)

        @pl.when(early)
        def _():
            prefetch(nxt, step + 1, before)

        r_tiles(d_half, d_tiles)
        keep = idx < N_OWN
        part_rows = ROWS // 4
        for h in range(4):
            rws = pl.ds(h * part_rows, part_rows)
            q = lax.rsqrt(jnp.sum(ring[0, rws, pl.ds(0, 128)], axis=-1, keepdims=True) * (1.0 / d) + EPS)
            mean = q * jnp.sum(ring[1, rws, pl.ds(0, 128)], axis=-1, keepdims=True) * (1.0 / d)
            qqm = q * q * mean
            for k in range(d // 128):
                lanes = pl.ds(k * 128, 128)
                xk = rb[1, rws, lanes].astype(F32)
                drk = gp[rws, lanes]
                dhk = main[slot, rws, lanes].astype(F32)
                main[slot, rws, lanes] = (dhk + (q * (drk * gain[:, lanes]) - xk * qqm)).astype(BF16)
                part = jnp.sum((drk * (xk * q)).reshape(part_rows // 8, 8, 128), axis=0)
                dgp[:, lanes] += jnp.where(keep, part, 0.0)

        @pl.when(sid > 0)
        def _():
            remote(main.at[slot], dh_all.at[rows, :], slot_snd.at[slot], dh_rcv.at[idx],
                   stage=jnp.maximum(sid - 1, 0)).start()

        load_gp(nxt, hi=d)

        @pl.when(idx == N_CHAIN - 1)
        def _():
            remote(dgp, dgr, dg_snd, dg_rcv, data=other).start()

            @pl.when(last)
            def _():
                red = lossacc[:, pl.ds(0, 128)]
                for k in range(1, d // 128):
                    red = red + lossacc[:, pl.ds(k * 128, 128)]
                lossred[...] = red
                for hop in range(1, 4):
                    remote(lossred, lossbuf.at[me_y], loss_snd.at[hop - 1], loss_rcv.at[me_y], stage=3 - hop).start()
                for hop in range(4):
                    remote(lossred, lossbuf.at[me_y], loss_snd.at[3 + hop], loss_rcv.at[me_y],
                           data=other, stage=3 - hop).start()

    def finish(b3, b2, b1):
        @pl.when(fields(b1)[0] == AUX)
        def _():
            u_out(1, pl.ds(0, ROWS)).wait()

        for back, code in ((3, b3), (2, b2), (1, b1)):
            wait_slot_send(code, (n_items - back) % 3)

        def end_relays(k, carry):
            relay_r(k).wait_send()
            relay_dh(k).wait_send()
            return carry

        lax.fori_loop(0, N_EXCH, end_relays, 0)

        @pl.when(first)
        def _():
            share_x.wait_send()

        @pl.when(last)
        def _():
            share_y.wait_send()

        dg_copy = remote(dgp, dgr, dg_snd, dg_rcv, data=other)
        dg_copy.wait_send()
        dg_copy.wait_recv()
        dg_out[...] = jnp.sum(dgp[...] + dgr[...], axis=0, keepdims=True)

        @pl.when(last)
        def _():
            for hop in range(7):
                remote(lossred, lossbuf.at[me_y], loss_snd.at[hop], loss_rcv.at[me_y], data=other).wait_send()
            lossbuf[me_y] = lossred[...]

        @pl.when(jnp.logical_not(last))
        def _():
            local(lossred, lossbuf.at[me_y], loss_rcv.at[me_y]).wait()

        local(lossred, lossbuf.at[other], loss_rcv.at[other]).wait()
        loss_out[0] = jnp.sum(lossbuf[0] + lossbuf[1]) / (tok_total * d)

    def item(step, carry):
        b3, b2, b1, cur = carry
        nxt = decode(step + 1)
        kind, idx, ready = fields(cur)
        slot = lax.rem(step, 3)
        early = fields(nxt)[2] & (step + 1 < n_items)
        after_aux = fields(b1)[0] == AUX
        rows = rows_of(jnp.where(kind == AUX, other * N_OWN + idx, own_chunk(idx)))

        @pl.when(step == n_items)
        def _():
            finish(b3, b2, b1)

        @pl.when(jnp.logical_not(ready))
        def _():
            prefetch(cur, step, b3)

        @pl.when(kind == PRE)
        def _():
            run_pre(step, idx, slot, nxt, early, b2, b1)

        @pl.when((kind == FWD) | (kind == AUX))
        def _():
            up_phase(step, kind, idx, slot, rows)

        @pl.when(kind == FWD)
        def _():
            down_phase(step, idx, slot, nxt, early, b2, after_aux)

        @pl.when((kind == BWD) | (kind == AUX))
        def _():
            back_phase(step, kind, idx, slot, rows, nxt, early, b2, after_aux)

        @pl.when(kind == BWD)
        def _():
            grad_phase(step, idx, slot, rows, nxt, early, b2)

        return b2, b1, cur, nxt

    none = jnp.int32(NONE)
    lax.fori_loop(0, n_items + 1, item, (none, none, none, decode(0)))


def grads_kernel(r_all, u_all, da_all, dh_all, d_up, d_down, pool, outs, held_ld, ring_ld, out_st):
    n_stream, n_held = u_all.shape[1] // TILE, dh_all.shape[1] // TILE
    n_ring = 3
    cols = lambda k: pl.ds(pl.multiple_of(k * TILE, TILE), TILE)

    def load_held(phase, j):
        src = dh_all if phase == 0 else r_all
        return pltpu.make_async_copy(src.at[:, cols(j)], pool.at[n_ring + phase * n_held + j], held_ld.at[phase, j])

    def load_ring(phase, k, slot):
        src = u_all if phase == 0 else da_all
        return pltpu.make_async_copy(src.at[:, cols(k)], pool.at[slot], ring_ld.at[slot])

    def store(phase, k, j, half):
        dst = d_down.at[cols(k), cols(j)] if phase == 0 else d_up.at[cols(j), cols(k)]
        return pltpu.make_async_copy(outs.at[half, j], dst, out_st.at[half, j])

    def body(count, carry):
        second = count >= n_stream
        k = lax.rem(count, n_stream)
        slot, half = lax.rem(count, n_ring), lax.rem(count, 2)
        load_ring(0, 0, slot).wait()
        ahead, next_k = lax.rem(count + 2, n_ring), lax.rem(count + 2, n_stream)

        @pl.when(count + 2 < n_stream)
        def _():
            load_ring(0, next_k, ahead).start()

        @pl.when((count + 2 >= n_stream) & (count + 2 < 2 * n_stream))
        def _():
            load_ring(1, next_k, ahead).start()

        for phase, at in ((0, 0), (1, n_stream)):
            @pl.when(count == at)
            def _():
                for j in range(n_held):
                    load_held(phase, j).wait()

        @pl.when(count == 1)
        def _():
            for j in range(n_held):
                load_held(1, j).start()

        @pl.when(count >= 2)
        def _():
            for j in range(n_held):
                store(0, 0, j, half).wait()

        for j in range(n_held):
            left = jnp.where(second, n_ring + n_held + j, slot)
            right = jnp.where(second, slot, n_ring + j)
            outs[half, j] = lax.dot_general(pool[left], pool[right], ROW_DIMS, preferred_element_type=F32)

        for phase in range(2):
            @pl.when(second if phase else jnp.logical_not(second))
            def _():
                for j in range(n_held):
                    store(phase, k, j, half).start()

        return carry

    load_ring(0, 0, 0).start()
    for j in range(n_held):
        load_held(0, j).start()
    load_ring(0, 1, 1).start()
    lax.fori_loop(0, 2 * n_stream, body, 0)
    for half in range(2):
        for j in range(n_held):
            store(0, 0, j, half).wait()


def encode(order):
    return tuple("FBAP".index(name[0]) + 4 * int(name[1:].rstrip("~")) + 64 * int(not name.endswith("~")) for name in order)


def solution(mesh):
    n_data = mesh.shape["data"]
    orders = tuple(encode(order) for order in ORDERS)

    def local_step(x_in, y_tgt, w_up, w_down, gain):
        n_micro, tokens, d = x_in.shape
        ff = w_up.shape[2]
        own = n_micro * tokens
        total = n_data * own
        x_rows, y_rows = x_in.reshape(own, d), y_tgt.reshape(own, d)
        hbm = pl.BlockSpec(memory_space=pl.ANY)
        vmem = pl.BlockSpec(memory_space=pltpu.VMEM)
        dma, sem = pltpu.SemaphoreType.DMA, pltpu.SemaphoreType.DMA(())
        out = pl.pallas_call(
            functools.partial(chain_kernel, orders, total),
            out_shape=(
                jax.ShapeDtypeStruct((total, d), BF16),
                jax.ShapeDtypeStruct((total, ff), BF16),
                jax.ShapeDtypeStruct((total, ff), BF16),
                jax.ShapeDtypeStruct((total, d), BF16),
                jax.ShapeDtypeStruct((N_CHAIN * ROWS, ff), F32),
                jax.ShapeDtypeStruct((N_CHAIN * ROWS, d), BF16),
                jax.ShapeDtypeStruct((ROWS, d), BF16),
                jax.ShapeDtypeStruct((1, d), F32),
                jax.ShapeDtypeStruct((1,), F32),
            ),
            in_specs=[hbm, hbm, hbm, hbm, vmem],
            out_specs=[hbm] * 7 + [vmem, pl.BlockSpec(memory_space=pltpu.SMEM)],
            scratch_shapes=[
                pltpu.VMEM((d, ff), BF16),
                pltpu.VMEM((ff, d), BF16),
                pltpu.VMEM((3, ROWS, d), BF16),
                pltpu.VMEM((2, ROWS, d), BF16),
                pltpu.VMEM((ROWS, ff), F32),
                pltpu.VMEM((2, ROWS, ff), BF16),
                pltpu.VMEM((2, ROWS, TILE), F32),
                pltpu.VMEM((8, d), F32),
                pltpu.VMEM((8, d), F32),
                pltpu.VMEM((8, d), F32),
                pltpu.VMEM((8, 128), F32),
                pltpu.VMEM((2, 8, 128), F32),
                dma((3,)), dma((3,)), dma((2,)), sem, sem, sem, dma((2,)), sem,
                dma((N_CHAIN + N_PRE,)), dma((N_CHAIN,)), dma((N_EXCH,)), dma((N_EXCH,)), sem, sem, dma((2,)),
                dma((3,)), dma((N_EXCH,)), dma((N_EXCH,)), sem, sem, dma((7,)),
            ],
            compiler_params=pltpu.CompilerParams(has_side_effects=True, vmem_limit_bytes=67043328),
            name="chain",
        )(x_rows, y_rows, w_up[0], w_down[0], gain)
        r_all, u_all, da_all, dh_all = out[:4]
        n_held = d // TILE
        d_up, d_down = pl.pallas_call(
            grads_kernel,
            out_shape=(jax.ShapeDtypeStruct((d, ff), F32), jax.ShapeDtypeStruct((ff, d), F32)),
            in_specs=[hbm] * 4,
            out_specs=[hbm] * 2,
            scratch_shapes=[
                pltpu.VMEM((3 + 2 * n_held, total, TILE), BF16),
                pltpu.VMEM((2, n_held, TILE, TILE), F32),
                dma((2, n_held)), dma((3,)), dma((2, n_held)),
            ],
            compiler_params=pltpu.CompilerParams(vmem_limit_bytes=67043328),
            name="grads",
        )(r_all, u_all, da_all, dh_all)
        return d_up[None], d_down[None], out[7], out[8]

    return jax.shard_map(local_step, mesh=mesh, in_specs=(P(("part", "data"), None, None), P(("part", "data"), None, None), P("stage", None, None), P("stage", None, None), P("stage", None)), out_specs=(P(("part", "stage"), None, None), P(("part", "stage"), None, None), P(("part", "stage"), None), P("part")), check_vma=False)
```

```python
import functools

import jax
import jax.numpy as jnp
from jax import lax
from jax.experimental import pallas as pl
from jax.experimental.pallas import tpu as pltpu
from jax.sharding import PartitionSpec as P

MESH = pl.DeviceIdType.MESH
EPS = 1e-6
C0 = 0.7978845608028654
C1 = 0.044715
ROWS = 256
HALF = ROWS // 2
TILE = 512
FWD, BWD, AUX, PRE = 0, 1, 2, 3
NONE = 64 * 17
LAST_DIMS = (((1,), (1,)), ((), ()))
ROW_DIMS = (((0,), (0,)), ((), ()))
F32 = jnp.float32
BF16 = jnp.bfloat16

ORDERS = (
    (
        "P0~", "P1", "P2", "P3", "F2", "F3", "F4", "F5", "F6",
        "F7", "B0~", "F8", "B1~", "A0", "A1", "B2~", "A2~", "B3",
        "B4", "A3~", "B5", "A4", "B6", "A5", "A6", "B7", "B8",
    ),
    (
        "P0~", "P1~", "P2", "P3", "F2~", "F3~", "F4~", "B0~", "F5",
        "F6", "B1~", "A0", "F7", "B2", "F8", "B3", "B4~", "A1",
        "B5~", "A2", "B6", "A3", "A4", "B7", "B8", "A5", "A6",
    ),
    (
        "P0~", "P1~", "P2~", "P3~", "B0~", "F2", "F3", "B1", "F4",
        "B2", "F5", "B3", "F6", "B4", "F7", "B5", "F8", "B6",
        "A0", "A1", "B7", "B8", "A2", "A3", "A4", "A5", "A6",
    ),
    (
        "P0~", "P1~", "B0", "P2", "P3", "B1", "F2~", "B2", "F3",
        "B3", "F4", "B4", "F5", "B5", "F6", "B6", "F7", "B7",
        "F8", "B8", "A0", "A1", "A2", "A3", "A4", "A5", "A6",
    ),
)
N_CHAIN = 9
N_OWN = 8
N_EXCH = 7
N_PRE = 2
N_AHEAD = 4


def gelu_and_grad(pre):
    sq = pre * pre
    th = jnp.tanh(pre * (C0 + (C0 * C1) * sq))
    cdf = 0.5 + 0.5 * th
    grad = cdf + (pre * (C0 + (3.0 * C0 * C1) * sq)) * (cdf * (1.0 - th))
    return pre * cdf, grad


def chain_kernel(orders, tok_total, x_in, y_tgt, w_up, w_down, gain, r_all, u_all, da_all, dh_all, gp_all, x_land, y_land,
                 dg_out, loss_out, w1, w2, main, rb, gp, ub, ring, dgp, dgr, lossacc, lossred, lossbuf,
                 w_ld, main_ld, rb_ld, r_sem, gp_o, gp_i, u_sem, dh_o, x_rcv, dh_rcv, rr_rcv, dd_rcv, y_rcv, dg_rcv, loss_rcv,
                 slot_snd, rr_snd, dd_snd, red_snd, dg_snd, loss_snd):
    n_items = len(orders[0])
    ff, d = w_down.shape
    me_y = lax.axis_index("data")
    sid = lax.axis_index("stage")
    other = 1 - me_y
    first, last = sid == 0, sid == 3
    f_tiles, d_tiles = ff // TILE, d // TILE
    cols = lambda k: pl.ds(k * TILE, TILE)

    def rows_of(chunk):
        return pl.ds(pl.multiple_of(chunk * ROWS, ROWS), ROWS)

    def own_chunk(idx):
        return jnp.where(idx < N_OWN, me_y * N_OWN + idx, other * N_OWN + idx - (N_CHAIN - N_OWN))

    def decode(step):
        code = jnp.int32(NONE)
        for stage_k, seq in enumerate(orders):
            val = jnp.int32(NONE)
            for step_k, item in enumerate(seq):
                val = jnp.where(step == step_k, item, val)
            code = jnp.where(sid == stage_k, val, code)
        return code

    def fields(code):
        kind, idx = lax.rem(code, 4), lax.rem(code // 4, 16)
        return jnp.where(code >= NONE, -1, kind), idx, lax.rem(code // 64, 2) == 1

    def local(src, dst, sem):
        return pltpu.make_async_copy(src, dst, sem)

    def remote(src, dst, snd, rcv, **to):
        return pltpu.make_async_remote_copy(src, dst, snd, rcv, device_id=to, device_id_type=MESH)

    def relay_r(k):
        rows = rows_of(me_y * N_OWN + k)
        return remote(r_all.at[rows, :], r_all.at[rows, :], rr_snd.at[k], rr_rcv.at[k], data=other)

    def relay_dh(k):
        rows = rows_of(me_y * N_OWN + k)
        return remote(dh_all.at[rows, :], dh_all.at[rows, :], dd_snd.at[k], dd_rcv.at[k], data=other)

    def u_out(which, rows):
        dst = u_all if which == 0 else da_all
        return local(ub.at[which], dst.at[rows, :], u_sem.at[which])

    def sends(code):
        kind = fields(code)[0]
        return (((kind == FWD) | (kind == PRE)) & (sid < 3)) | ((kind == BWD) & (sid > 0))

    def wait_slot_send(code, slot):
        pre = fields(code)[0] == PRE

        @pl.when(sends(code) & pre)
        def _():
            half = pl.ds(0, HALF)
            remote(main.at[slot, half, :], x_land.at[half, :], slot_snd.at[slot], x_rcv.at[0], data=other).wait_send()

        @pl.when(sends(code) & jnp.logical_not(pre))
        def _():
            remote(main.at[slot], x_land.at[pl.ds(0, ROWS), :], slot_snd.at[slot], x_rcv.at[0], data=other).wait_send()

    def load_x(idx, dst, sem):
        @pl.when(first & (idx < N_OWN))
        def _():
            local(x_in.at[rows_of(jnp.minimum(idx, N_OWN - 1)), :], dst, sem).start()

        @pl.when(jnp.logical_not(first & (idx < N_OWN)))
        def _():
            local(x_land.at[rows_of(idx), :], dst, sem).start()

    def prefetch(code, step, before, waited=None):
        kind, idx, _ = fields(code)
        slot = lax.rem(step, 3)

        if waited is None:
            wait_slot_send(before, slot)
        else:
            @pl.when(jnp.logical_not(waited))
            def _():
                wait_slot_send(before, slot)

        @pl.when(kind == PRE)
        def _():
            half = pl.ds(pl.multiple_of(idx * HALF, HALF), HALF)
            dst = main.at[slot, in_chunk(idx), :]

            @pl.when(first & (step > 0))
            def _():
                local(x_in.at[half, :], dst, main_ld.at[slot]).start()

            @pl.when(jnp.logical_not(first))
            def _():
                local(x_land.at[half, :], x_land.at[half, :], x_rcv.at[pre_sem(idx)]).wait()
                local(x_land.at[half, :], dst, main_ld.at[slot]).start()

        @pl.when(kind == FWD)
        def _():
            @pl.when(jnp.logical_not(first & (idx < N_OWN)))
            def _():
                local(x_land.at[rows_of(idx), :], x_land.at[rows_of(idx), :], x_rcv.at[idx]).wait()

            load_x(idx, main.at[slot], main_ld.at[slot])

        @pl.when((kind == BWD) & jnp.logical_not(last))
        def _():
            rows = rows_of(own_chunk(idx))
            local(dh_all.at[rows, :], dh_all.at[rows, :], dh_rcv.at[idx]).wait()
            local(dh_all.at[rows, :], main.at[slot], main_ld.at[slot]).start()

            @pl.when(idx < N_EXCH)
            def _():
                relay_dh(idx).start()

            @pl.when((sid < 2) & (idx < N_EXCH - N_AHEAD))
            def _():
                relay_r(jnp.minimum(idx + N_AHEAD, N_EXCH - 1)).start()

        @pl.when(kind == AUX)
        def _():
            rows = rows_of(other * N_OWN + idx)
            local(r_all.at[rows, :], r_all.at[rows, :], rr_rcv.at[idx]).wait()
            local(r_all.at[rows, :], rb.at[0], rb_ld.at[0]).start()
            local(dh_all.at[rows, :], dh_all.at[rows, :], dd_rcv.at[idx]).wait()
            local(dh_all.at[rows, :], main.at[slot], main_ld.at[slot]).start()

    def pre_sem(idx):
        return jnp.where(lax.rem(idx, 2) == 0, N_CHAIN + idx // 2, idx // 2)

    def in_chunk(idx):
        return pl.ds(pl.multiple_of(lax.rem(idx, 2) * HALF, HALF), HALF)

    def load_gp(code, lo=0, hi=None):
        kind, idx, _ = fields(code)
        lanes = pl.ds(lo, (hi or ff) - lo)

        @pl.when((kind == BWD) & jnp.logical_not(last))
        def _():
            for k in range(4):
                quarter = pl.ds(pl.multiple_of(idx * ROWS + k * (ROWS // 4), ROWS // 4), ROWS // 4)
                local(gp_all.at[quarter, lanes], gp.at[pl.ds(k * (ROWS // 4), ROWS // 4), lanes], gp_i).start()

    def normalise(slot, rws):
        acc = jnp.zeros((rws.size, 128), F32)
        for k in range(d // 128):
            xk = main[slot, rws, pl.ds(k * 128, 128)].astype(F32)
            acc = acc + xk * xk
        q = lax.rsqrt(jnp.sum(acc, axis=-1, keepdims=True) * (1.0 / d) + EPS)
        for k in range(d // 128):
            lanes = pl.ds(k * 128, 128)
            rb[0, rws, lanes] = (main[slot, rws, lanes].astype(F32) * q * gain[:, lanes]).astype(BF16)

    def up_tiles(rws):
        n = rws.size
        for k in range(f_tiles + 1):
            if k > 0:
                act, grad = gelu_and_grad(ring[(k - 1) % 2, pl.ds(0, n), :])
                ub[0, rws, cols(k - 1)] = act.astype(BF16)
                gp[rws, cols(k - 1)] = grad
            if k < f_tiles:
                ring[k % 2, pl.ds(0, n), :] = jnp.dot(rb[0, rws, :], w1[:, cols(k)], preferred_element_type=F32)

    def down_tiles(lo, hi, slot, out_slot, rws, count):
        n, slab = rws.size, HALF // 2

        def done(k):
            for r in range(n // slab):
                at = rws.start + r * slab
                rw = pl.ds(at if isinstance(at, int) else pl.multiple_of(at, slab), slab)
                upd = ring[k % 2, pl.ds(r * slab, slab), :]
                h = (main[slot, rw, cols(k)].astype(F32) + upd).astype(BF16)
                err = h.astype(F32) - rb[1, rw, cols(k)].astype(F32)
                main[out_slot, rw, cols(k)] = jnp.where(last, (err * (1.0 / tok_total)).astype(BF16), h)
                part = jnp.sum((err * err).reshape(slab // 8, 8, TILE), axis=0)
                lossacc[:, cols(k)] += jnp.where(count, part, 0.0)

        for k in range(lo, hi + 1):
            if k > lo:
                done(k - 1)
            if k < hi:
                ring[k % 2, pl.ds(0, n), :] = jnp.dot(ub[0, rws, :], w2[:, cols(k)], preferred_element_type=F32)

    @pl.when(first)
    def _():
        half = pl.ds(0, HALF)
        local(x_in.at[half, :], main.at[0, half, :], main_ld.at[0]).start()

    for k in range(2):
        half = pl.ds(k * (d // 2), d // 2)
        local(w_up.at[half, :], w1.at[half, :], w_ld.at[0]).start()
    def load_w2(k):
        lanes = pl.ds(k * (d // 2), d // 2)
        return local(w_down.at[:, lanes], w2.at[:, lanes], w_ld.at[1 + k])

    @pl.when(jnp.logical_not(first))
    def _():
        for k in range(2):
            load_w2(k).start()

    barrier = pltpu.get_barrier_semaphore()
    for far in range(2):
        for hop in range(int(far == 0), 4):
            pl.semaphore_signal(barrier, inc=1, device_id={"data": other if far else me_y, "stage": lax.rem(sid + hop, 4)},
                                device_id_type=MESH)
    pl.semaphore_wait(barrier, 7)

    share = pl.ds(N_EXCH * ROWS, ROWS)
    share_x = remote(x_in.at[share, :], x_land.at[pl.ds(N_OWN * ROWS, ROWS), :], red_snd, x_rcv.at[N_OWN], data=other)
    share_y = remote(y_tgt.at[share, :], y_land, red_snd, y_rcv, data=other)

    @pl.when(first)
    def _():
        share_x.start()

    @pl.when(last)
    def _():
        share_y.start()

    dgp[...] = jnp.zeros_like(dgp)
    lossacc[...] = jnp.zeros_like(lossacc)
    for k in range(d // 128):
        rb[1, :, pl.ds(k * 128, 128)] = jnp.zeros((ROWS, 128), BF16)

    d_half = d_tiles // 2

    def send_half(k, slot, rws, land, sem):
        lanes = pl.ds(k * (d // 2), d // 2)

        @pl.when(sid < 3)
        def _():
            remote(main.at[slot, rws, lanes], x_land.at[land, lanes], slot_snd.at[slot], x_rcv.at[sem],
                   stage=jnp.minimum(sid + 1, 3)).start()

    def run_pre(step, idx, slot, nxt, early, before, prev):
        rws, at = in_chunk(idx), pl.ds(pl.multiple_of(idx * HALF, HALF), HALF)
        odd = lax.rem(idx, 2)
        own = pl.ds(pl.multiple_of(me_y * N_OWN * ROWS + idx * HALF, HALF), HALF)

        @pl.when(last)
        def _():
            local(y_tgt.at[at, :], rb.at[1, rws, :], rb_ld.at[1]).start()

        local(x_in.at[pl.ds(0, HALF), :], main.at[slot, rws, :], main_ld.at[slot]).wait()
        for h in range(2):
            normalise(slot, pl.ds(pl.multiple_of(odd * HALF + h * (HALF // 2), HALF // 2), HALF // 2))
        r_out = local(rb.at[0, rws, :], r_all.at[own, :], r_sem)
        r_out.start()

        @pl.when(step == 0)
        def _():
            local(w_up, w1, w_ld.at[0]).wait()

        @pl.when((step == 0) & first)
        def _():
            for k in range(2):
                load_w2(k).start()

        up_tiles(rws)
        r_out.wait()

        @pl.when(odd == 1)
        def _():
            relay_r(idx // 2).start()

        act_out = local(ub.at[0, rws, :], u_all.at[own, :], u_sem.at[0])
        act_out.start()
        gp_out = local(gp.at[rws, :], gp_all.at[at, :], gp_o)

        @pl.when(jnp.logical_not(last))
        def _():
            gp_out.start()

        @pl.when(step == 0)
        def _():
            load_w2(0).wait()

        @pl.when(last)
        def _():
            local(y_tgt.at[at, :], rb.at[1, rws, :], rb_ld.at[1]).wait()

        out_slot = jnp.where(last, lax.rem(step + 2 - odd, 3), slot)

        @pl.when(last & (odd == 0))
        def _():
            wait_slot_send(prev, out_slot)

        down_tiles(0, d_half, slot, out_slot, rws, last)
        send_half(0, slot, rws, at, pre_sem(idx))
        act_out.wait()

        @pl.when(jnp.logical_not(last))
        def _():
            gp_out.wait()

        load_gp(nxt)

        @pl.when(early)
        def _():
            prefetch(nxt, step + 1, before, last & (odd == 1))

        @pl.when(step == 0)
        def _():
            load_w2(1).wait()

        down_tiles(d_half, d_tiles, slot, out_slot, rws, last)
        send_half(1, slot, rws, at, pre_sem(idx))

    def up_phase(step, kind, idx, slot, rows):
        fwd = kind == FWD
        r_out = local(rb.at[0], r_all.at[rows, :], r_sem)
        gp_out = local(gp, gp_all.at[rows_of(idx), :], gp_o)

        @pl.when(fwd & last)
        def _():
            @pl.when(idx < N_OWN)
            def _():
                local(y_tgt.at[rows_of(jnp.minimum(idx, N_OWN - 1)), :], rb.at[1], rb_ld.at[1]).start()

            @pl.when(idx >= N_OWN)
            def _():
                local(y_land, y_land, y_rcv).wait()
                local(y_land, rb.at[1], rb_ld.at[1]).start()

        @pl.when(fwd)
        def _():
            local(x_in.at[pl.ds(0, ROWS), :], main.at[slot], main_ld.at[slot]).wait()
            for h in range(4):
                normalise(slot, pl.ds(h * (ROWS // 4), ROWS // 4))
            r_out.start()

        @pl.when(kind == AUX)
        def _():
            local(r_all.at[pl.ds(0, ROWS), :], rb.at[0], rb_ld.at[0]).wait()

        up_tiles(pl.ds(0, ROWS))
        u_out(0, rows).start()

        @pl.when(fwd)
        def _():
            r_out.wait()

        @pl.when(fwd & (idx < jnp.where(sid < 2, N_AHEAD, N_EXCH)))
        def _():
            relay_r(jnp.minimum(idx, N_EXCH - 1)).start()

        @pl.when(fwd & jnp.logical_not(last))
        def _():
            gp_out.start()

    def down_phase(step, idx, slot, nxt, early, before, after_aux):
        @pl.when(last)
        def _():
            local(y_land, rb.at[1], rb_ld.at[1]).wait()

        out_slot = jnp.where(last, lax.rem(step + 1, 3), slot)
        count = last & (idx < N_OWN)
        every = pl.ds(0, ROWS)
        down_tiles(0, d_half, slot, out_slot, every, count)
        send_half(0, slot, every, rows_of(idx), idx)
        u_out(0, every).wait()

        @pl.when(after_aux)
        def _():
            u_out(1, every).wait()

        @pl.when(jnp.logical_not(last))
        def _():
            local(gp, gp_all.at[every, :], gp_o).wait()

        load_gp(nxt)

        @pl.when(early)
        def _():
            prefetch(nxt, step + 1, before)

        down_tiles(d_half, d_tiles, slot, out_slot, every, count)
        send_half(1, slot, every, rows_of(idx), idx)

    def back_phase(step, kind, idx, slot, rows, nxt, early, before, after_aux):
        bwd, aux = kind == BWD, kind == AUX
        dh_out = local(main.at[slot], dh_all.at[rows, :], dh_o)

        @pl.when(bwd)
        def _():
            load_x(idx, rb.at[1], rb_ld.at[1])

        @pl.when(bwd & last)
        def _():
            dh_out.start()

        @pl.when(aux | jnp.logical_not(last))
        def _():
            local(x_in.at[pl.ds(0, ROWS), :], main.at[slot], main_ld.at[slot]).wait()

        @pl.when(bwd & jnp.logical_not(last))
        def _():
            local(gp_all.at[pl.ds(0, ROWS), :], gp, gp_i).wait()

        @pl.when(after_aux)
        def _():
            u_out(1, rows).wait()

        @pl.when(aux & early)
        def _():
            prefetch(nxt, step + 1, before)

        for k in range(f_tiles):
            du = lax.dot_general(main[slot], w2[cols(k), :], LAST_DIMS, preferred_element_type=F32)
            ub[1, :, cols(k)] = (du * gp[:, cols(k)]).astype(BF16)
        u_out(1, rows).start()

        @pl.when(aux)
        def _():
            u_out(0, rows).wait()
            load_gp(nxt)

        @pl.when(bwd & last)
        def _():
            dh_out.wait()

        @pl.when(bwd & last & (idx < N_EXCH))
        def _():
            relay_dh(jnp.minimum(idx, N_EXCH - 1)).start()

    def grad_phase(step, idx, slot, rows, nxt, early, before):
        load_gp(nxt, lo=d)

        @pl.when(early)
        def _():
            prefetch(nxt, step + 1, before)

        local(x_land.at[pl.ds(0, ROWS), :], rb.at[1], rb_ld.at[1]).wait()

        sums = pl.ds(0, 128)
        keep = jnp.where(idx < N_OWN, 0, 1)
        part_rows = ROWS // 4

        def inv_rms():
            for h in range(4):
                rws = pl.ds(h * part_rows, part_rows)
                acc = jnp.zeros((part_rows, 128), F32)
                for k in range(d // 128):
                    xk = rb[1, rws, pl.ds(k * 128, 128)].astype(F32)
                    acc = acc + xk * xk
                q = lax.rsqrt(jnp.sum(acc, axis=-1, keepdims=True) * (1.0 / d) + EPS)
                ring[0, rws, sums] = jnp.broadcast_to(q, (part_rows, 128))

        def r_done(k):
            for h in range(4):
                rws = pl.ds(h * part_rows, part_rows)
                pr = jnp.zeros((part_rows, 128), F32)
                for j in range(TILE // 128):
                    lanes = pl.ds(k * TILE + j * 128, 128)
                    unit = rb[1, rws, lanes].astype(F32) * ring[0, rws, sums]
                    prod = gp[rws, lanes] * unit
                    pr = pr + prod * gain[:, lanes]
                    dgp[keep, :, lanes] += jnp.sum(prod.reshape(part_rows // 8, 8, 128), axis=0)
                ring[1, rws, sums] = pr if k == 0 else ring[1, rws, sums] + pr

        def r_tiles(lo, hi):
            for k in range(lo, hi + 1):
                if k > lo:
                    r_done(k - 1)
                if k < hi:
                    gp[:, cols(k)] = lax.dot_general(ub[1], w1[cols(k), :], LAST_DIMS, preferred_element_type=F32)
                if k == 0:
                    inv_rms()

        r_tiles(0, d_tiles)
        for h in range(4):
            rws = pl.ds(h * part_rows, part_rows)
            q = ring[0, rws, sums]
            q_mean = q * (jnp.sum(ring[1, rws, sums], axis=-1, keepdims=True) * (1.0 / d))
            for k in range(d // 128):
                lanes = pl.ds(k * 128, 128)
                dx = q * (gp[rws, lanes] * gain[:, lanes] - rb[1, rws, lanes].astype(F32) * q_mean)
                main[slot, rws, lanes] = (main[slot, rws, lanes].astype(F32) + dx).astype(BF16)

        @pl.when(sid > 0)
        def _():
            remote(main.at[slot], dh_all.at[rows, :], slot_snd.at[slot], dh_rcv.at[idx],
                   stage=jnp.maximum(sid - 1, 0)).start()

        load_gp(nxt, hi=d)
        u_out(1, rows).wait()

        @pl.when(idx == N_OWN - 1)
        def _():
            remote(dgp.at[0], dgr, dg_snd, dg_rcv, data=other).start()

            @pl.when(last)
            def _():
                red = lossacc[:, pl.ds(0, 128)]
                for k in range(1, d // 128):
                    red = red + lossacc[:, pl.ds(k * 128, 128)]
                lossred[...] = red
                for hop in range(1, 4):
                    remote(lossred, lossbuf.at[me_y], loss_snd.at[hop - 1], loss_rcv.at[me_y], stage=3 - hop).start()
                for hop in range(4):
                    remote(lossred, lossbuf.at[me_y], loss_snd.at[3 + hop], loss_rcv.at[me_y],
                           data=other, stage=3 - hop).start()

    def finish(b3, b2, b1):
        @pl.when(fields(b1)[0] == AUX)
        def _():
            u_out(1, pl.ds(0, ROWS)).wait()

        for back, code in ((3, b3), (2, b2), (1, b1)):
            wait_slot_send(code, (n_items - back) % 3)

        def end_relays(k, carry):
            relay_r(k).wait_send()
            relay_dh(k).wait_send()
            return carry

        lax.fori_loop(0, N_EXCH, end_relays, 0)

        @pl.when(first)
        def _():
            share_x.wait_send()

        @pl.when(last)
        def _():
            share_y.wait_send()

        dg_copy = remote(dgp.at[0], dgr, dg_snd, dg_rcv, data=other)
        dg_copy.wait_send()
        dg_copy.wait_recv()
        dg_out[...] = jnp.sum(dgp[0] + dgr[...], axis=0, keepdims=True)

        @pl.when(last)
        def _():
            for hop in range(7):
                remote(lossred, lossbuf.at[me_y], loss_snd.at[hop], loss_rcv.at[me_y], data=other).wait_send()
            lossbuf[me_y] = lossred[...]

        @pl.when(jnp.logical_not(last))
        def _():
            local(lossred, lossbuf.at[me_y], loss_rcv.at[me_y]).wait()

        local(lossred, lossbuf.at[other], loss_rcv.at[other]).wait()
        loss_out[0] = jnp.sum(lossbuf[0] + lossbuf[1]) / (tok_total * d)

    def item(step, carry):
        b3, b2, b1, cur = carry
        nxt = decode(step + 1)
        kind, idx, ready = fields(cur)
        slot = lax.rem(step, 3)
        early = fields(nxt)[2] & (step + 1 < n_items)
        after_aux = fields(b1)[0] == AUX
        rows = rows_of(jnp.where(kind == AUX, other * N_OWN + idx, own_chunk(idx)))

        @pl.when(step == n_items)
        def _():
            finish(b3, b2, b1)

        @pl.when(jnp.logical_not(ready))
        def _():
            prefetch(cur, step, b3)

        @pl.when(kind == PRE)
        def _():
            run_pre(step, idx, slot, nxt, early, b2, b1)

        @pl.when((kind == FWD) | (kind == AUX))
        def _():
            up_phase(step, kind, idx, slot, rows)

        @pl.when(kind == FWD)
        def _():
            down_phase(step, idx, slot, nxt, early, b2, after_aux)

        @pl.when((kind == BWD) | (kind == AUX))
        def _():
            back_phase(step, kind, idx, slot, rows, nxt, early, b2, after_aux)

        @pl.when(kind == BWD)
        def _():
            grad_phase(step, idx, slot, rows, nxt, early, b2)

        return b2, b1, cur, nxt

    none = jnp.int32(NONE)
    lax.fori_loop(0, n_items + 1, item, (none, none, none, decode(0)))


def grads_kernel(r_all, u_all, da_all, dh_all, dg, loss, d_up, d_down, dg_out, loss_out, pool, outs, held_ld, ring_ld, out_st, small):
    n_stream, n_held = u_all.shape[1] // TILE, dh_all.shape[1] // TILE
    n_ring = 3
    cols = lambda k: pl.ds(pl.multiple_of(k * TILE, TILE), TILE)

    def load_held(phase, j):
        src = dh_all if phase == 0 else r_all
        return pltpu.make_async_copy(src.at[:, cols(j)], pool.at[n_ring + phase * n_held + j], held_ld.at[phase, j])

    def load_ring(phase, k, slot):
        src = u_all if phase == 0 else da_all
        return pltpu.make_async_copy(src.at[:, cols(k)], pool.at[slot], ring_ld.at[slot])

    def store(phase, k, j, half):
        dst = d_down.at[cols(k), cols(j)] if phase == 0 else d_up.at[cols(j), cols(k)]
        return pltpu.make_async_copy(outs.at[half, j], dst, out_st.at[half, j])

    def body(count, carry):
        second = count >= n_stream
        k = lax.rem(count, n_stream)
        slot, half = lax.rem(count, n_ring), lax.rem(count, 2)
        load_ring(0, 0, slot).wait()
        ahead, next_k = lax.rem(count + 2, n_ring), lax.rem(count + 2, n_stream)

        @pl.when(count + 2 < n_stream)
        def _():
            load_ring(0, next_k, ahead).start()

        @pl.when((count + 2 >= n_stream) & (count + 2 < 2 * n_stream))
        def _():
            load_ring(1, next_k, ahead).start()

        for phase, at in ((0, 0), (1, n_stream)):
            @pl.when(count == at)
            def _():
                for j in range(n_held):
                    load_held(phase, j).wait()

        @pl.when(count == 1)
        def _():
            for j in range(n_held):
                load_held(1, j).start()

        @pl.when(count >= 2)
        def _():
            for j in range(n_held):
                store(0, 0, j, half).wait()

        for j in range(n_held):
            left = jnp.where(second, n_ring + n_held + j, slot)
            right = jnp.where(second, slot, n_ring + j)
            outs[half, j] = lax.dot_general(pool[left], pool[right], ROW_DIMS, preferred_element_type=F32)

        for phase in range(2):
            @pl.when(second if phase else jnp.logical_not(second))
            def _():
                for j in range(n_held):
                    store(phase, k, j, half).start()

        return carry

    load_ring(0, 0, 0).start()
    for j in range(n_held):
        load_held(0, j).start()
    load_ring(0, 1, 1).start()
    pass_dg = pltpu.make_async_copy(dg, dg_out, small.at[0])
    pass_loss = pltpu.make_async_copy(loss, loss_out, small.at[1])
    pass_dg.start()
    pass_loss.start()
    lax.fori_loop(0, 2 * n_stream, body, 0)
    pass_dg.wait()
    pass_loss.wait()
    for half in range(2):
        for j in range(n_held):
            store(0, 0, j, half).wait()


def encode(order):
    return tuple("FBAP".index(name[0]) + 4 * int(name[1:].rstrip("~")) + 64 * int(not name.endswith("~")) for name in order)


def solution(mesh):
    n_data = mesh.shape["data"]
    orders = tuple(encode(order) for order in ORDERS)

    def local_step(x_in, y_tgt, w_up, w_down, gain):
        n_micro, tokens, d = x_in.shape
        ff = w_up.shape[2]
        own = n_micro * tokens
        total = n_data * own
        x_rows, y_rows = x_in.reshape(own, d), y_tgt.reshape(own, d)
        hbm = pl.BlockSpec(memory_space=pl.ANY)
        vmem = pl.BlockSpec(memory_space=pltpu.VMEM)
        dma, sem = pltpu.SemaphoreType.DMA, pltpu.SemaphoreType.DMA(())
        out = pl.pallas_call(
            functools.partial(chain_kernel, orders, total),
            out_shape=(
                jax.ShapeDtypeStruct((total, d), BF16),
                jax.ShapeDtypeStruct((total, ff), BF16),
                jax.ShapeDtypeStruct((total, ff), BF16),
                jax.ShapeDtypeStruct((total, d), BF16),
                jax.ShapeDtypeStruct((N_CHAIN * ROWS, ff), F32),
                jax.ShapeDtypeStruct((N_CHAIN * ROWS, d), BF16),
                jax.ShapeDtypeStruct((ROWS, d), BF16),
                jax.ShapeDtypeStruct((1, d), F32),
                jax.ShapeDtypeStruct((1,), F32),
            ),
            in_specs=[hbm, hbm, hbm, hbm, vmem],
            out_specs=[hbm] * 7 + [vmem, pl.BlockSpec(memory_space=pltpu.SMEM)],
            scratch_shapes=[
                pltpu.VMEM((d, ff), BF16),
                pltpu.VMEM((ff, d), BF16),
                pltpu.VMEM((3, ROWS, d), BF16),
                pltpu.VMEM((2, ROWS, d), BF16),
                pltpu.VMEM((ROWS, ff), F32),
                pltpu.VMEM((2, ROWS, ff), BF16),
                pltpu.VMEM((2, ROWS, TILE), F32),
                pltpu.VMEM((2, 8, d), F32),
                pltpu.VMEM((8, d), F32),
                pltpu.VMEM((8, d), F32),
                pltpu.VMEM((8, 128), F32),
                pltpu.VMEM((2, 8, 128), F32),
                dma((3,)), dma((3,)), dma((2,)), sem, sem, sem, dma((2,)), sem,
                dma((N_CHAIN + N_PRE,)), dma((N_CHAIN,)), dma((N_EXCH,)), dma((N_EXCH,)), sem, sem, dma((2,)),
                dma((3,)), dma((N_EXCH,)), dma((N_EXCH,)), sem, sem, dma((7,)),
            ],
            compiler_params=pltpu.CompilerParams(collective_id=0, has_side_effects=True, vmem_limit_bytes=67043328),
            name="chain",
        )(x_rows, y_rows, w_up[0], w_down[0], gain)
        n_held = d // TILE
        d_up, d_down, d_gain, loss = pl.pallas_call(
            grads_kernel,
            out_shape=(
                jax.ShapeDtypeStruct((d, ff), F32),
                jax.ShapeDtypeStruct((ff, d), F32),
                jax.ShapeDtypeStruct((1, d), F32),
                jax.ShapeDtypeStruct((1,), F32),
            ),
            in_specs=[hbm] * 6,
            out_specs=[hbm] * 4,
            scratch_shapes=[
                pltpu.VMEM((3 + 2 * n_held, total, TILE), BF16),
                pltpu.VMEM((2, n_held, TILE, TILE), F32),
                dma((2, n_held)), dma((3,)), dma((2, n_held)), dma((2,)),
            ],
            compiler_params=pltpu.CompilerParams(vmem_limit_bytes=67043328),
            name="grads",
        )(*out[:4], *out[7:])
        return d_up[None], d_down[None], d_gain, loss

    return jax.shard_map(local_step, mesh=mesh, in_specs=(P(("part", "data"), None, None), P(("part", "data"), None, None), P("stage", None, None), P("stage", None, None), P("stage", None)), out_specs=(P(("part", "stage"), None, None), P(("part", "stage"), None, None), P(("part", "stage"), None), P("part")), check_vma=False)
```

```python
import functools

import jax
import jax.numpy as jnp
from jax import lax
from jax.experimental import pallas as pl
from jax.experimental.pallas import tpu as pltpu
from jax.sharding import PartitionSpec as P

MESH = pl.DeviceIdType.MESH
EPS = 1e-6
C0 = 0.7978845608028654
C1 = 0.044715
ROWS = 256
HALF = ROWS // 2
TILE = 512
FWD, BWD, AUX, PRE = 0, 1, 2, 3
NONE = 64 * 17
LAST_DIMS = (((1,), (1,)), ((), ()))
ROW_DIMS = (((0,), (0,)), ((), ()))
F32 = jnp.float32
BF16 = jnp.bfloat16

ORDERS = (
    (
        "P0~", "P1", "P2", "P3", "F2", "F3", "F4", "F5", "F6",
        "F7", "B0~", "F8", "B1~", "A0", "A1", "B2~", "A2~", "B3",
        "B4", "A3~", "B5", "A4", "B6", "A5", "A6", "B7", "B8",
    ),
    (
        "P0~", "P1~", "P2", "P3", "F2~", "F3~", "F4~", "B0~", "F5",
        "F6", "B1~", "A0", "F7", "B2", "F8", "B3", "B4~", "A1",
        "B5~", "A2", "B6", "A3", "A4", "B7", "B8", "A5", "A6",
    ),
    (
        "P0~", "P1~", "P2~", "P3~", "B0~", "F2", "F3", "B1", "F4",
        "B2", "F5", "B3", "F6", "B4", "F7", "B5", "F8", "B6",
        "A0", "A1", "B7", "B8", "A2", "A3", "A4", "A5", "A6",
    ),
    (
        "P0~", "P1~", "B0", "P2", "P3", "B1", "F2~", "B2", "F3",
        "B3", "F4", "B4", "F5", "B5", "F6", "B6", "F7", "B7",
        "F8", "B8", "A0", "A1", "A2", "A3", "A4", "A5", "A6",
    ),
)
N_CHAIN = 9
N_OWN = 8
N_EXCH = 7
N_PRE = 2
N_AHEAD = 4


def gelu_and_grad(pre):
    sq = pre * pre
    th = jnp.tanh(pre * (C0 + (C0 * C1) * sq))
    cdf = 0.5 + 0.5 * th
    grad = cdf + (pre * (C0 + (3.0 * C0 * C1) * sq)) * (cdf * (1.0 - th))
    return pre * cdf, grad


def chain_kernel(orders, tok_total, x_in, y_tgt, w_up, w_down, gain, r_all, u_all, da_all, dh_all, gp_all, x_land, y_land,
                 dg_out, loss_out, w1, w2, main, rb, gp, ub, ring, dgp, dgr, lossacc, lossred, lossbuf,
                 w_ld, main_ld, rb_ld, r_sem, gp_o, gp_i, u_sem, dh_o, x_rcv, dh_rcv, rr_rcv, dd_rcv, y_rcv, dg_rcv, loss_rcv,
                 slot_snd, rr_snd, dd_snd, red_snd, dg_snd, loss_snd):
    n_items = len(orders[0])
    ff, d = w_down.shape
    me_y = lax.axis_index("data")
    sid = lax.axis_index("stage")
    other = 1 - me_y
    first, last = sid == 0, sid == 3
    f_tiles, d_tiles = ff // TILE, d // TILE
    cols = lambda k: pl.ds(k * TILE, TILE)

    def rows_of(chunk):
        return pl.ds(pl.multiple_of(chunk * ROWS, ROWS), ROWS)

    def own_chunk(idx):
        return jnp.where(idx < N_OWN, me_y * N_OWN + idx, other * N_OWN + idx - (N_CHAIN - N_OWN))

    def decode(step):
        code = jnp.int32(NONE)
        for stage_k, seq in enumerate(orders):
            val = jnp.int32(NONE)
            for step_k, item in enumerate(seq):
                val = jnp.where(step == step_k, item, val)
            code = jnp.where(sid == stage_k, val, code)
        return code

    def fields(code):
        kind, idx = lax.rem(code, 4), lax.rem(code // 4, 16)
        return jnp.where(code >= NONE, -1, kind), idx, lax.rem(code // 64, 2) == 1

    def local(src, dst, sem):
        return pltpu.make_async_copy(src, dst, sem)

    def remote(src, dst, snd, rcv, **to):
        return pltpu.make_async_remote_copy(src, dst, snd, rcv, device_id=to, device_id_type=MESH)

    def relay_r(k):
        rows = rows_of(me_y * N_OWN + k)
        return remote(r_all.at[rows, :], r_all.at[rows, :], rr_snd.at[k], rr_rcv.at[k], data=other)

    def relay_dh(k):
        rows = rows_of(me_y * N_OWN + k)
        return remote(dh_all.at[rows, :], dh_all.at[rows, :], dd_snd.at[k], dd_rcv.at[k], data=other)

    def u_out(which, rows):
        dst = u_all if which == 0 else da_all
        return local(ub.at[which], dst.at[rows, :], u_sem.at[which])

    def sends(code):
        kind = fields(code)[0]
        return (((kind == FWD) | (kind == PRE)) & (sid < 3)) | ((kind == BWD) & (sid > 0))

    def wait_slot_send(code, slot):
        pre = fields(code)[0] == PRE

        @pl.when(sends(code) & pre)
        def _():
            half = pl.ds(0, HALF)
            remote(main.at[slot, half, :], x_land.at[half, :], slot_snd.at[slot], x_rcv.at[0], data=other).wait_send()

        @pl.when(sends(code) & jnp.logical_not(pre))
        def _():
            remote(main.at[slot], x_land.at[pl.ds(0, ROWS), :], slot_snd.at[slot], x_rcv.at[0], data=other).wait_send()

    def load_x(idx, dst, sem):
        @pl.when(first & (idx < N_OWN))
        def _():
            local(x_in.at[rows_of(jnp.minimum(idx, N_OWN - 1)), :], dst, sem).start()

        @pl.when(jnp.logical_not(first & (idx < N_OWN)))
        def _():
            local(x_land.at[rows_of(idx), :], dst, sem).start()

    def prefetch(code, step, before, waited=None):
        kind, idx, _ = fields(code)
        slot = lax.rem(step, 3)

        if waited is None:
            wait_slot_send(before, slot)
        else:
            @pl.when(jnp.logical_not(waited))
            def _():
                wait_slot_send(before, slot)

        @pl.when(kind == PRE)
        def _():
            half = pl.ds(pl.multiple_of(idx * HALF, HALF), HALF)
            dst = main.at[slot, in_chunk(idx), :]

            @pl.when(first & (step > 0))
            def _():
                local(x_in.at[half, :], dst, main_ld.at[slot]).start()

            @pl.when(jnp.logical_not(first))
            def _():
                local(x_land.at[half, :], x_land.at[half, :], x_rcv.at[pre_sem(idx)]).wait()
                local(x_land.at[half, :], dst, main_ld.at[slot]).start()

        @pl.when(kind == FWD)
        def _():
            @pl.when(jnp.logical_not(first & (idx < N_OWN)))
            def _():
                local(x_land.at[rows_of(idx), :], x_land.at[rows_of(idx), :], x_rcv.at[idx]).wait()

            load_x(idx, main.at[slot], main_ld.at[slot])

        @pl.when((kind == BWD) & jnp.logical_not(last))
        def _():
            rows = rows_of(own_chunk(idx))
            local(dh_all.at[rows, :], dh_all.at[rows, :], dh_rcv.at[idx]).wait()
            local(dh_all.at[rows, :], main.at[slot], main_ld.at[slot]).start()

            @pl.when(idx < N_EXCH)
            def _():
                relay_dh(idx).start()

            @pl.when((sid < 2) & (idx < N_EXCH - N_AHEAD))
            def _():
                relay_r(jnp.minimum(idx + N_AHEAD, N_EXCH - 1)).start()

        @pl.when(kind == AUX)
        def _():
            rows = rows_of(other * N_OWN + idx)
            local(r_all.at[rows, :], r_all.at[rows, :], rr_rcv.at[idx]).wait()
            local(r_all.at[rows, :], rb.at[0], rb_ld.at[0]).start()
            local(dh_all.at[rows, :], dh_all.at[rows, :], dd_rcv.at[idx]).wait()
            local(dh_all.at[rows, :], main.at[slot], main_ld.at[slot]).start()

    def pre_sem(idx):
        return jnp.where(lax.rem(idx, 2) == 0, N_CHAIN + idx // 2, idx // 2)

    def in_chunk(idx):
        return pl.ds(pl.multiple_of(lax.rem(idx, 2) * HALF, HALF), HALF)

    def load_gp(code, lo=0, hi=None):
        kind, idx, _ = fields(code)
        lanes = pl.ds(lo, (hi or ff) - lo)

        @pl.when((kind == BWD) & jnp.logical_not(last))
        def _():
            for k in range(4):
                quarter = pl.ds(pl.multiple_of(idx * ROWS + k * (ROWS // 4), ROWS // 4), ROWS // 4)
                local(gp_all.at[quarter, lanes], gp.at[pl.ds(k * (ROWS // 4), ROWS // 4), lanes], gp_i).start()

    def normalise(slot, rws):
        acc = jnp.zeros((rws.size, 128), F32)
        for k in range(d // 128):
            xk = main[slot, rws, pl.ds(k * 128, 128)].astype(F32)
            acc = acc + xk * xk
        q = lax.rsqrt(jnp.sum(acc, axis=-1, keepdims=True) * (1.0 / d) + EPS)
        for k in range(d // 128):
            lanes = pl.ds(k * 128, 128)
            rb[0, rws, lanes] = (main[slot, rws, lanes].astype(F32) * q * gain[:, lanes]).astype(BF16)

    def up_tiles(rws):
        n = rws.size
        for k in range(f_tiles + 1):
            if k > 0:
                act, grad = gelu_and_grad(ring[(k - 1) % 2, pl.ds(0, n), :])
                ub[0, rws, cols(k - 1)] = act.astype(BF16)
                gp[rws, cols(k - 1)] = grad
            if k < f_tiles:
                ring[k % 2, pl.ds(0, n), :] = jnp.dot(rb[0, rws, :], w1[:, cols(k)], preferred_element_type=F32)

    def down_tiles(lo, hi, slot, out_slot, rws, count):
        n, slab = rws.size, HALF // 2

        def done(k):
            for r in range(n // slab):
                at = rws.start + r * slab
                rw = pl.ds(at if isinstance(at, int) else pl.multiple_of(at, slab), slab)
                upd = ring[k % 2, pl.ds(r * slab, slab), :]
                h = (main[slot, rw, cols(k)].astype(F32) + upd).astype(BF16)
                err = h.astype(F32) - rb[1, rw, cols(k)].astype(F32)
                main[out_slot, rw, cols(k)] = jnp.where(last, (err * (1.0 / tok_total)).astype(BF16), h)
                part = jnp.sum((err * err).reshape(slab // 8, 8, TILE), axis=0)
                lossacc[:, cols(k)] += jnp.where(count, part, 0.0)

        for k in range(lo, hi + 1):
            if k > lo:
                done(k - 1)
            if k < hi:
                ring[k % 2, pl.ds(0, n), :] = jnp.dot(ub[0, rws, :], w2[:, cols(k)], preferred_element_type=F32)

    @pl.when(first)
    def _():
        half = pl.ds(0, HALF)
        local(x_in.at[half, :], main.at[0, half, :], main_ld.at[0]).start()

    for k in range(2):
        half = pl.ds(k * (d // 2), d // 2)
        local(w_up.at[half, :], w1.at[half, :], w_ld.at[0]).start()
    def load_w2(k):
        lanes = pl.ds(k * (d // 2), d // 2)
        return local(w_down.at[:, lanes], w2.at[:, lanes], w_ld.at[1 + k])

    @pl.when(jnp.logical_not(first))
    def _():
        for k in range(2):
            load_w2(k).start()

    barrier = pltpu.get_barrier_semaphore()
    for far in range(2):
        for hop in range(int(far == 0), 4):
            pl.semaphore_signal(barrier, inc=1, device_id={"data": other if far else me_y, "stage": lax.rem(sid + hop, 4)},
                                device_id_type=MESH)
    pl.semaphore_wait(barrier, 7)

    share = pl.ds(N_EXCH * ROWS, ROWS)
    share_x = remote(x_in.at[share, :], x_land.at[pl.ds(N_OWN * ROWS, ROWS), :], red_snd, x_rcv.at[N_OWN], data=other)
    share_y = remote(y_tgt.at[share, :], y_land, red_snd, y_rcv, data=other)

    @pl.when(first)
    def _():
        share_x.start()

    @pl.when(last)
    def _():
        share_y.start()

    dgp[...] = jnp.zeros_like(dgp)
    lossacc[...] = jnp.zeros_like(lossacc)
    for k in range(d // 128):
        rb[1, :, pl.ds(k * 128, 128)] = jnp.zeros((ROWS, 128), BF16)

    d_half = d_tiles // 2

    def send_half(k, slot, rws, land, sem):
        lanes = pl.ds(k * (d // 2), d // 2)

        @pl.when(sid < 3)
        def _():
            remote(main.at[slot, rws, lanes], x_land.at[land, lanes], slot_snd.at[slot], x_rcv.at[sem],
                   stage=jnp.minimum(sid + 1, 3)).start()

    def run_pre(step, idx, slot, nxt, early, before, prev):
        rws, at = in_chunk(idx), pl.ds(pl.multiple_of(idx * HALF, HALF), HALF)
        odd = lax.rem(idx, 2)
        own = pl.ds(pl.multiple_of(me_y * N_OWN * ROWS + idx * HALF, HALF), HALF)

        @pl.when(last)
        def _():
            local(y_tgt.at[at, :], rb.at[1, rws, :], rb_ld.at[1]).start()

        local(x_in.at[pl.ds(0, HALF), :], main.at[slot, rws, :], main_ld.at[slot]).wait()
        for h in range(2):
            normalise(slot, pl.ds(pl.multiple_of(odd * HALF + h * (HALF // 2), HALF // 2), HALF // 2))
        r_out = local(rb.at[0, rws, :], r_all.at[own, :], r_sem)
        r_out.start()

        @pl.when(step == 0)
        def _():
            local(w_up, w1, w_ld.at[0]).wait()

        @pl.when((step == 0) & first)
        def _():
            for k in range(2):
                load_w2(k).start()

        up_tiles(rws)
        r_out.wait()

        @pl.when(odd == 1)
        def _():
            relay_r(idx // 2).start()

        act_out = local(ub.at[0, rws, :], u_all.at[own, :], u_sem.at[0])
        act_out.start()
        gp_out = local(gp.at[rws, :], gp_all.at[at, :], gp_o)

        @pl.when(jnp.logical_not(last))
        def _():
            gp_out.start()

        @pl.when(step == 0)
        def _():
            load_w2(0).wait()

        @pl.when(last)
        def _():
            local(y_tgt.at[at, :], rb.at[1, rws, :], rb_ld.at[1]).wait()

        out_slot = jnp.where(last, lax.rem(step + 2 - odd, 3), slot)

        @pl.when(last & (odd == 0))
        def _():
            wait_slot_send(prev, out_slot)

        down_tiles(0, d_half, slot, out_slot, rws, last)
        send_half(0, slot, rws, at, pre_sem(idx))
        act_out.wait()

        @pl.when(jnp.logical_not(last))
        def _():
            gp_out.wait()

        load_gp(nxt)

        @pl.when(early)
        def _():
            prefetch(nxt, step + 1, before, last & (odd == 1))

        @pl.when(step == 0)
        def _():
            load_w2(1).wait()

        down_tiles(d_half, d_tiles, slot, out_slot, rws, last)
        send_half(1, slot, rws, at, pre_sem(idx))

    def up_phase(step, kind, idx, slot, rows):
        fwd = kind == FWD
        r_out = local(rb.at[0], r_all.at[rows, :], r_sem)
        gp_out = local(gp, gp_all.at[rows_of(idx), :], gp_o)

        @pl.when(fwd & last)
        def _():
            @pl.when(idx < N_OWN)
            def _():
                local(y_tgt.at[rows_of(jnp.minimum(idx, N_OWN - 1)), :], rb.at[1], rb_ld.at[1]).start()

            @pl.when(idx >= N_OWN)
            def _():
                local(y_land, y_land, y_rcv).wait()
                local(y_land, rb.at[1], rb_ld.at[1]).start()

        @pl.when(fwd)
        def _():
            local(x_in.at[pl.ds(0, ROWS), :], main.at[slot], main_ld.at[slot]).wait()
            for h in range(4):
                normalise(slot, pl.ds(h * (ROWS // 4), ROWS // 4))
            r_out.start()

        @pl.when(kind == AUX)
        def _():
            local(r_all.at[pl.ds(0, ROWS), :], rb.at[0], rb_ld.at[0]).wait()

        up_tiles(pl.ds(0, ROWS))
        u_out(0, rows).start()

        @pl.when(fwd)
        def _():
            r_out.wait()

        @pl.when(fwd & (idx < jnp.where(sid < 2, N_AHEAD, N_EXCH)))
        def _():
            relay_r(jnp.minimum(idx, N_EXCH - 1)).start()

        @pl.when(fwd & jnp.logical_not(last))
        def _():
            gp_out.start()

    def down_phase(step, idx, slot, nxt, early, before, after_aux):
        @pl.when(last)
        def _():
            local(y_land, rb.at[1], rb_ld.at[1]).wait()

        out_slot = jnp.where(last, lax.rem(step + 1, 3), slot)
        count = last & (idx < N_OWN)
        every = pl.ds(0, ROWS)
        down_tiles(0, d_half, slot, out_slot, every, count)
        send_half(0, slot, every, rows_of(idx), idx)
        u_out(0, every).wait()

        @pl.when(after_aux)
        def _():
            u_out(1, every).wait()

        @pl.when(jnp.logical_not(last))
        def _():
            local(gp, gp_all.at[every, :], gp_o).wait()

        load_gp(nxt)

        @pl.when(early)
        def _():
            prefetch(nxt, step + 1, before)

        down_tiles(d_half, d_tiles, slot, out_slot, every, count)
        send_half(1, slot, every, rows_of(idx), idx)

    def back_phase(step, kind, idx, slot, rows, nxt, early, before, after_aux):
        bwd, aux = kind == BWD, kind == AUX
        dh_out = local(main.at[slot], dh_all.at[rows, :], dh_o)

        @pl.when(bwd)
        def _():
            load_x(idx, rb.at[1], rb_ld.at[1])

        @pl.when(bwd & last)
        def _():
            dh_out.start()

        @pl.when(aux | jnp.logical_not(last))
        def _():
            local(x_in.at[pl.ds(0, ROWS), :], main.at[slot], main_ld.at[slot]).wait()

        @pl.when(bwd & jnp.logical_not(last))
        def _():
            local(gp_all.at[pl.ds(0, ROWS), :], gp, gp_i).wait()

        @pl.when(after_aux)
        def _():
            u_out(1, rows).wait()

        @pl.when(aux & early)
        def _():
            prefetch(nxt, step + 1, before)

        for k in range(f_tiles):
            du = lax.dot_general(main[slot], w2[cols(k), :], LAST_DIMS, preferred_element_type=F32)
            ub[1, :, cols(k)] = (du * gp[:, cols(k)]).astype(BF16)
        u_out(1, rows).start()

        @pl.when(aux)
        def _():
            u_out(0, rows).wait()
            load_gp(nxt)

        @pl.when(bwd & last)
        def _():
            dh_out.wait()

        @pl.when(bwd & last & (idx < N_EXCH))
        def _():
            relay_dh(jnp.minimum(idx, N_EXCH - 1)).start()

    def grad_phase(step, idx, slot, rows, nxt, early, before):
        load_gp(nxt, lo=d)

        @pl.when(early)
        def _():
            prefetch(nxt, step + 1, before)

        local(x_land.at[pl.ds(0, ROWS), :], rb.at[1], rb_ld.at[1]).wait()

        sums = pl.ds(0, 128)
        keep = jnp.where(idx < N_OWN, 0, 1)
        part_rows = ROWS // 4

        def inv_rms():
            for h in range(4):
                rws = pl.ds(h * part_rows, part_rows)
                acc = jnp.zeros((part_rows, 128), F32)
                for k in range(d // 128):
                    xk = rb[1, rws, pl.ds(k * 128, 128)].astype(F32)
                    acc = acc + xk * xk
                q = lax.rsqrt(jnp.sum(acc, axis=-1, keepdims=True) * (1.0 / d) + EPS)
                ring[0, rws, sums] = jnp.broadcast_to(q, (part_rows, 128))

        def r_done(k):
            for h in range(4):
                rws = pl.ds(h * part_rows, part_rows)
                pr = jnp.zeros((part_rows, 128), F32)
                for j in range(TILE // 128):
                    lanes = pl.ds(k * TILE + j * 128, 128)
                    unit = rb[1, rws, lanes].astype(F32) * ring[0, rws, sums]
                    prod = gp[rws, lanes] * unit
                    pr = pr + prod * gain[:, lanes]
                    dgp[keep, :, lanes] += jnp.sum(prod.reshape(part_rows // 8, 8, 128), axis=0)
                ring[1, rws, sums] = pr if k == 0 else ring[1, rws, sums] + pr

        def r_tiles(lo, hi):
            for k in range(lo, hi + 1):
                if k > lo:
                    r_done(k - 1)
                if k < hi:
                    gp[:, cols(k)] = lax.dot_general(ub[1], w1[cols(k), :], LAST_DIMS, preferred_element_type=F32)
                if k == 0:
                    inv_rms()

        r_tiles(0, d_tiles)
        @pl.when(sid > 0)
        def _():
            for h in range(4):
                rws = pl.ds(h * part_rows, part_rows)
                q = ring[0, rws, sums]
                q_mean = q * (jnp.sum(ring[1, rws, sums], axis=-1, keepdims=True) * (1.0 / d))
                for k in range(d // 128):
                    lanes = pl.ds(k * 128, 128)
                    dx = q * (gp[rws, lanes] * gain[:, lanes] - rb[1, rws, lanes].astype(F32) * q_mean)
                    main[slot, rws, lanes] = (main[slot, rws, lanes].astype(F32) + dx).astype(BF16)

            remote(main.at[slot], dh_all.at[rows, :], slot_snd.at[slot], dh_rcv.at[idx],
                   stage=jnp.maximum(sid - 1, 0)).start()

        load_gp(nxt, hi=d)
        u_out(1, rows).wait()

        @pl.when(idx == N_OWN - 1)
        def _():
            remote(dgp.at[0], dgr, dg_snd, dg_rcv, data=other).start()

            @pl.when(last)
            def _():
                red = lossacc[:, pl.ds(0, 128)]
                for k in range(1, d // 128):
                    red = red + lossacc[:, pl.ds(k * 128, 128)]
                lossred[...] = red
                for hop in range(1, 4):
                    remote(lossred, lossbuf.at[me_y], loss_snd.at[hop - 1], loss_rcv.at[me_y], stage=3 - hop).start()
                for hop in range(4):
                    remote(lossred, lossbuf.at[me_y], loss_snd.at[3 + hop], loss_rcv.at[me_y],
                           data=other, stage=3 - hop).start()

    def finish(b3, b2, b1):
        @pl.when(fields(b1)[0] == AUX)
        def _():
            u_out(1, pl.ds(0, ROWS)).wait()

        for back, code in ((3, b3), (2, b2), (1, b1)):
            wait_slot_send(code, (n_items - back) % 3)

        def end_relays(k, carry):
            relay_r(k).wait_send()
            relay_dh(k).wait_send()
            return carry

        lax.fori_loop(0, N_EXCH, end_relays, 0)

        @pl.when(first)
        def _():
            share_x.wait_send()

        @pl.when(last)
        def _():
            share_y.wait_send()

        dg_copy = remote(dgp.at[0], dgr, dg_snd, dg_rcv, data=other)
        dg_copy.wait_send()
        dg_copy.wait_recv()
        dg_out[...] = jnp.sum(dgp[0] + dgr[...], axis=0, keepdims=True)

        @pl.when(last)
        def _():
            for hop in range(7):
                remote(lossred, lossbuf.at[me_y], loss_snd.at[hop], loss_rcv.at[me_y], data=other).wait_send()
            lossbuf[me_y] = lossred[...]

        @pl.when(jnp.logical_not(last))
        def _():
            local(lossred, lossbuf.at[me_y], loss_rcv.at[me_y]).wait()

        local(lossred, lossbuf.at[other], loss_rcv.at[other]).wait()
        loss_out[0] = jnp.sum(lossbuf[0] + lossbuf[1]) / (tok_total * d)

    def item(step, carry):
        b3, b2, b1, cur = carry
        nxt = decode(step + 1)
        kind, idx, ready = fields(cur)
        slot = lax.rem(step, 3)
        early = fields(nxt)[2] & (step + 1 < n_items)
        after_aux = fields(b1)[0] == AUX
        rows = rows_of(jnp.where(kind == AUX, other * N_OWN + idx, own_chunk(idx)))

        @pl.when(step == n_items)
        def _():
            finish(b3, b2, b1)

        @pl.when(jnp.logical_not(ready))
        def _():
            prefetch(cur, step, b3)

        @pl.when(kind == PRE)
        def _():
            run_pre(step, idx, slot, nxt, early, b2, b1)

        @pl.when((kind == FWD) | (kind == AUX))
        def _():
            up_phase(step, kind, idx, slot, rows)

        @pl.when(kind == FWD)
        def _():
            down_phase(step, idx, slot, nxt, early, b2, after_aux)

        @pl.when((kind == BWD) | (kind == AUX))
        def _():
            back_phase(step, kind, idx, slot, rows, nxt, early, b2, after_aux)

        @pl.when(kind == BWD)
        def _():
            grad_phase(step, idx, slot, rows, nxt, early, b2)

        return b2, b1, cur, nxt

    none = jnp.int32(NONE)
    lax.fori_loop(0, n_items + 1, item, (none, none, none, decode(0)))


def grads_kernel(r_all, u_all, da_all, dh_all, dg, loss, d_up, d_down, dg_out, loss_out, pool, outs, held_ld, ring_ld, out_st, small):
    n_stream, n_held = u_all.shape[1] // TILE, dh_all.shape[1] // TILE
    n_ring = 3
    cols = lambda k: pl.ds(pl.multiple_of(k * TILE, TILE), TILE)

    def load_held(phase, j):
        src = dh_all if phase == 0 else r_all
        return pltpu.make_async_copy(src.at[:, cols(j)], pool.at[n_ring + phase * n_held + j], held_ld.at[phase, j])

    def load_ring(phase, k, slot):
        src = u_all if phase == 0 else da_all
        return pltpu.make_async_copy(src.at[:, cols(k)], pool.at[slot], ring_ld.at[slot])

    def store(phase, k, j, half):
        dst = d_down.at[cols(k), cols(j)] if phase == 0 else d_up.at[cols(j), cols(k)]
        return pltpu.make_async_copy(outs.at[half, j], dst, out_st.at[half, j])

    def body(count, carry):
        second = count >= n_stream
        k = lax.rem(count, n_stream)
        slot, half = lax.rem(count, n_ring), lax.rem(count, 2)
        load_ring(0, 0, slot).wait()
        ahead, next_k = lax.rem(count + 2, n_ring), lax.rem(count + 2, n_stream)

        @pl.when(count + 2 < n_stream)
        def _():
            load_ring(0, next_k, ahead).start()

        @pl.when((count + 2 >= n_stream) & (count + 2 < 2 * n_stream))
        def _():
            load_ring(1, next_k, ahead).start()

        for phase, at in ((0, 0), (1, n_stream)):
            @pl.when(count == at)
            def _():
                for j in range(n_held):
                    load_held(phase, j).wait()

        @pl.when(count == 1)
        def _():
            for j in range(n_held):
                load_held(1, j).start()

        @pl.when(count >= 2)
        def _():
            for j in range(n_held):
                store(0, 0, j, half).wait()

        for j in range(n_held):
            left = jnp.where(second, n_ring + n_held + j, slot)
            right = jnp.where(second, slot, n_ring + j)
            outs[half, j] = lax.dot_general(pool[left], pool[right], ROW_DIMS, preferred_element_type=F32)

        for phase in range(2):
            @pl.when(second if phase else jnp.logical_not(second))
            def _():
                for j in range(n_held):
                    store(phase, k, j, half).start()

        return carry

    load_ring(0, 0, 0).start()
    for j in range(n_held):
        load_held(0, j).start()
    load_ring(0, 1, 1).start()
    pass_dg = pltpu.make_async_copy(dg, dg_out, small.at[0])
    pass_loss = pltpu.make_async_copy(loss, loss_out, small.at[1])
    pass_dg.start()
    pass_loss.start()
    lax.fori_loop(0, 2 * n_stream, body, 0)
    pass_dg.wait()
    pass_loss.wait()
    for half in range(2):
        for j in range(n_held):
            store(0, 0, j, half).wait()


def encode(order):
    return tuple("FBAP".index(name[0]) + 4 * int(name[1:].rstrip("~")) + 64 * int(not name.endswith("~")) for name in order)


def solution(mesh):
    n_data = mesh.shape["data"]
    orders = tuple(encode(order) for order in ORDERS)

    def local_step(x_in, y_tgt, w_up, w_down, gain):
        n_micro, tokens, d = x_in.shape
        ff = w_up.shape[2]
        own = n_micro * tokens
        total = n_data * own
        x_rows, y_rows = x_in.reshape(own, d), y_tgt.reshape(own, d)
        hbm = pl.BlockSpec(memory_space=pl.ANY)
        vmem = pl.BlockSpec(memory_space=pltpu.VMEM)
        dma, sem = pltpu.SemaphoreType.DMA, pltpu.SemaphoreType.DMA(())
        out = pl.pallas_call(
            functools.partial(chain_kernel, orders, total),
            out_shape=(
                jax.ShapeDtypeStruct((total, d), BF16),
                jax.ShapeDtypeStruct((total, ff), BF16),
                jax.ShapeDtypeStruct((total, ff), BF16),
                jax.ShapeDtypeStruct((total, d), BF16),
                jax.ShapeDtypeStruct((N_CHAIN * ROWS, ff), F32),
                jax.ShapeDtypeStruct((N_CHAIN * ROWS, d), BF16),
                jax.ShapeDtypeStruct((ROWS, d), BF16),
                jax.ShapeDtypeStruct((1, d), F32),
                jax.ShapeDtypeStruct((1,), F32),
            ),
            in_specs=[hbm, hbm, hbm, hbm, vmem],
            out_specs=[hbm] * 7 + [vmem, pl.BlockSpec(memory_space=pltpu.SMEM)],
            scratch_shapes=[
                pltpu.VMEM((d, ff), BF16),
                pltpu.VMEM((ff, d), BF16),
                pltpu.VMEM((3, ROWS, d), BF16),
                pltpu.VMEM((2, ROWS, d), BF16),
                pltpu.VMEM((ROWS, ff), F32),
                pltpu.VMEM((2, ROWS, ff), BF16),
                pltpu.VMEM((2, ROWS, TILE), F32),
                pltpu.VMEM((2, 8, d), F32),
                pltpu.VMEM((8, d), F32),
                pltpu.VMEM((8, d), F32),
                pltpu.VMEM((8, 128), F32),
                pltpu.VMEM((2, 8, 128), F32),
                dma((3,)), dma((3,)), dma((2,)), sem, sem, sem, dma((2,)), sem,
                dma((N_CHAIN + N_PRE,)), dma((N_CHAIN,)), dma((N_EXCH,)), dma((N_EXCH,)), sem, sem, dma((2,)),
                dma((3,)), dma((N_EXCH,)), dma((N_EXCH,)), sem, sem, dma((7,)),
            ],
            compiler_params=pltpu.CompilerParams(collective_id=0, has_side_effects=True, vmem_limit_bytes=67043328),
            name="chain",
        )(x_rows, y_rows, w_up[0], w_down[0], gain)
        n_held = d // TILE
        d_up, d_down, d_gain, loss = pl.pallas_call(
            grads_kernel,
            out_shape=(
                jax.ShapeDtypeStruct((d, ff), F32),
                jax.ShapeDtypeStruct((ff, d), F32),
                jax.ShapeDtypeStruct((1, d), F32),
                jax.ShapeDtypeStruct((1,), F32),
            ),
            in_specs=[hbm] * 6,
            out_specs=[hbm] * 4,
            scratch_shapes=[
                pltpu.VMEM((3 + 2 * n_held, total, TILE), BF16),
                pltpu.VMEM((2, n_held, TILE, TILE), F32),
                dma((2, n_held)), dma((3,)), dma((2, n_held)), dma((2,)),
            ],
            compiler_params=pltpu.CompilerParams(vmem_limit_bytes=67043328),
            name="grads",
        )(*out[:4], *out[7:])
        return d_up[None], d_down[None], d_gain, loss

    return jax.shard_map(local_step, mesh=mesh, in_specs=(P(("part", "data"), None, None), P(("part", "data"), None, None), P("stage", None, None), P("stage", None, None), P("stage", None)), out_specs=(P(("part", "stage"), None, None), P(("part", "stage"), None, None), P(("part", "stage"), None), P("part")), check_vma=False)
```
